16 devices in a mesh: rep: 2 (over y, z), dp: 8 (over x, core).
Axes of the slice: x: 4, y: 2, z: 1, core: 2. Of those that a mesh axis runs over, the one named last changes fastest.
The devices are a block of a 4x4x8 slice.
Arguments:
- x: bfloat16 [16, 2048, 640], P(('rep', 'dp')), parts along dimension 0
- dy: bfloat16 [16, 2048, 640], P(('rep', 'dp')), parts along dimension 0
- w_gate: bfloat16 [2, 640, 3200], replicated
- w_up: bfloat16 [2, 640, 3200], replicated
- w_down: bfloat16 [2, 3200, 640], replicated
- m_w_gate: float32 [2, 640, 3200], P(None, 'dp')
- m_w_up: float32 [2, 640, 3200], P(None, 'dp')
- m_w_down: float32 [2, 3200, 640], P(None, 'dp')
- v_w_gate: float32 [2, 640, 3200], P(None, 'dp')
- v_w_up: float32 [2, 640, 3200], P(None, 'dp')
- v_w_down: float32 [2, 3200, 640], P(None, 'dp')
Outputs:
- output 1: bfloat16 [4, 640, 3200], P('rep'), parts along dimension 0
- output 2: bfloat16 [4, 640, 3200], P('rep'), parts along dimension 0
- output 3: bfloat16 [4, 3200, 640], P('rep'), parts along dimension 0
- output 4: float32 [4, 640, 3200], P('rep', 'dp'), parts along dimension 0
- output 5: float32 [4, 640, 3200], P('rep', 'dp'), parts along dimension 0
- output 6: float32 [4, 3200, 640], P('rep', 'dp'), parts along dimension 0
- output 7: float32 [4, 640, 3200], P('rep', 'dp'), parts along dimension 0
- output 8: float32 [4, 640, 3200], P('rep', 'dp'), parts along dimension 0
- output 9: float32 [4, 3200, 640], P('rep', 'dp'), parts along dimension 0
There are 2 independent parts. The reference program is written for one: setup_inputs(seed, part) draws one part's arguments, and reference() takes and returns one part's arrays. A program takes and returns all parts, laid end to end along the dimension named above; an argument that names none is the same for every part.
All inputs are finite; a program needn't handle non-finite values.
Results may differ from the reference program's by a relative error of at most 0.022.
Values are sent between devices in bfloat16 or wider.
A program may use at most 768 MiB of HBM per device.

```python
import jax
import jax.numpy as jnp
from jax import lax

SEQUENCES = 8
TOKENS = 2048
D = 640
FF = 3200
LAYERS = 2
NAMES = ("w_gate", "w_up", "w_down")
SHAPES = {"w_gate": (LAYERS, D, FF), "w_up": (LAYERS, D, FF), "w_down": (LAYERS, FF, D)}


def bump(key, n, height):
    away = (jnp.arange(n, dtype=jnp.int32) - jax.random.randint(key, (), 0, n, jnp.int32)) % n
    return jnp.where(away < n // 8, height, 1.0)


def together(key, own, strength):
    shared = jax.random.normal(key, own.shape[1:], jnp.float32)
    return (own + strength * shared) * lax.rsqrt(1 + strength * strength)


def setup_inputs(seed: int = 0, part: int = 0) -> dict:
    kx, kdy, ka, kb, kz, kf, kh, kl, *keys = jax.random.split(jax.random.key(seed), 8 + 3 * len(NAMES))
    kx, kdy, ka, kb = (jax.random.fold_in(k, part) for k in (kx, kdy, ka, kb))
    kw, km, kv = (keys[i::3] for i in range(3))
    shape = (SEQUENCES, TOKENS, D)
    much_x, much_dy = jax.random.uniform(kz, (2,), jnp.float32, 0.0, 1.0)
    loud = 2.0 ** jax.random.uniform(jax.random.fold_in(kz, 1), (), jnp.float32, -1.0, 2.0)
    layers = 2.0 ** jax.random.uniform(kl, (LAYERS, 1, 1), jnp.float32, -1.0, 1.0)
    x = together(ka, jax.random.normal(kx, shape, jnp.float32), much_x) * bump(kf, D, 4.0)
    dy = together(kb, jax.random.normal(kdy, shape, jnp.float32), much_dy)
    drawn = {"x": x.astype(jnp.bfloat16), "dy": (loud * dy * (SEQUENCES * TOKENS) ** -0.5).astype(jnp.bfloat16)}
    for key, name in zip(kw, NAMES, strict=True):
        w = jax.random.normal(key, SHAPES[name], jnp.float32) * SHAPES[name][1] ** -0.5
        drawn[name] = (w * {"w_gate": 1.0, "w_up": bump(kh, FF, 4.0), "w_down": layers}[name]).astype(jnp.bfloat16)
    for key, name in zip(km, NAMES, strict=True):
        drawn[f"m_{name}"] = 0.1 * jax.random.normal(key, SHAPES[name], jnp.float32)
    for key, name in zip(kv, NAMES, strict=True):
        drawn[f"v_{name}"] = jax.random.uniform(key, SHAPES[name], jnp.float32, 0.005, 0.015)
    return drawn


def matmul(a, w):
    return jnp.dot(a, w, preferred_element_type=jnp.float32).astype(jnp.bfloat16)


def normed(h):
    wide = h.astype(jnp.float32)
    scale = lax.rsqrt(jnp.mean(wide**2, -1, keepdims=True) + 1e-6)
    return (wide * scale).astype(jnp.bfloat16)


def layer(h, w):
    a = normed(h)
    gate = jnp.dot(a, w["w_gate"], preferred_element_type=jnp.float32)
    up = jnp.dot(a, w["w_up"], preferred_element_type=jnp.float32)
    return h + matmul((jax.nn.silu(gate) * up).astype(jnp.bfloat16), w["w_down"])


def adamw(w, m, v, g):
    m = 0.9 * m + 0.1 * g
    v = 0.95 * v + 0.05 * g * g
    step = m * lax.rsqrt(v + 1e-8) + 0.1 * w
    return (w - 0.02 * step).astype(jnp.bfloat16), m, v


def clipped(gradients, sum_of_squares, count):
    factor = jnp.minimum(1.0, 0.5 * lax.rsqrt(sum_of_squares / count + 1e-30))
    return [g * factor for g in gradients]


def stack(weights, h):
    return lax.scan(lambda h, w: (layer(h, w), None), h, weights)[0]


def reference(x, dy, w_gate, w_up, w_down, m_w_gate, m_w_up, m_w_down, v_w_gate, v_w_up, v_w_down):
    weights = dict(zip(NAMES, (w_gate, w_up, w_down), strict=True))

    def take(so_far, sequence):
        h, by_y = sequence
        _, back = jax.vjp(lambda w: stack(w, h), weights)
        return jax.tree.map(lambda total, term: total + term.astype(jnp.float32), so_far, back(by_y)[0]), None

    none_yet = {name: jnp.zeros(w.shape, jnp.float32) for name, w in weights.items()}
    by_weights, _ = lax.scan(take, none_yet, (x, dy))
    gradients = [by_weights[name].astype(jnp.bfloat16).astype(jnp.float32) for name in NAMES]
    gradients = clipped(gradients, sum(jnp.sum(g * g) for g in gradients), sum(g.size for g in gradients))
    new = [
        adamw(w.astype(jnp.float32), m, v, g)
        for w, m, v, g in zip((w_gate, w_up, w_down), (m_w_gate, m_w_up, m_w_down), (v_w_gate, v_w_up, v_w_down), gradients, strict=True)
    ]
    return tuple(one[which] for which in range(3) for one in new)
```

```python
import jax
import jax.numpy as jnp
from jax import lax
from jax.sharding import PartitionSpec as P

NAMES = ("w_gate", "w_up", "w_down")


def matmul(a, w):
    return jnp.dot(a, w, preferred_element_type=jnp.float32).astype(jnp.bfloat16)


def normed(h):
    wide = h.astype(jnp.float32)
    scale = lax.rsqrt(jnp.mean(wide**2, -1, keepdims=True) + 1e-6)
    return (wide * scale).astype(jnp.bfloat16)


def layer(h, w):
    a = normed(h)
    gate = jnp.dot(a, w[0], preferred_element_type=jnp.float32)
    up = jnp.dot(a, w[1], preferred_element_type=jnp.float32)
    return h + matmul((jax.nn.silu(gate) * up).astype(jnp.bfloat16), w[2])


def adamw(w, m, v, g):
    m = 0.9 * m + 0.1 * g
    v = 0.95 * v + 0.05 * g * g
    step = m * lax.rsqrt(v + 1e-8) + 0.1 * w
    return (w - 0.02 * step).astype(jnp.bfloat16), m, v


def solution(mesh):
    dp = mesh.shape["dp"]

    def step(x, dy, *arrays):
        weights, m, v = (arrays[i : i + 3] for i in (0, 3, 6))
        layers = weights[0].shape[0]
        per_layer = [tuple(w[i] for w in weights) for i in range(layers)]

        def stack(per_layer, h):
            for w in per_layer:
                h = layer(h, w)
            return h

        _, back = jax.vjp(lambda w: stack(w, x[0]), per_layer)
        grads = back(dy[0])[0]
        me = lax.axis_index("dp")
        g = [[None] * layers for _ in weights]
        for i in reversed(range(layers)):
            for j in (2, 0, 1):
                g[j][i] = lax.psum_scatter(grads[i][j], "dp", scatter_dimension=0, tiled=True).astype(jnp.float32)
        total = lax.psum(sum(jnp.sum(t * t) for row in g for t in row), "dp")
        count = sum(w.size for w in weights)
        factor = jnp.minimum(1.0, 0.5 * lax.rsqrt(total / count + 1e-30))
        new_w, new_m, new_v = [], [], []
        for j, w in enumerate(weights):
            rows = m[j].shape[1]
            mine = lax.dynamic_slice_in_dim(w, me * rows, rows, 1).astype(jnp.float32)
            nw, nm, nv = adamw(mine, m[j], v[j], jnp.stack(g[j]) * factor)
            new_w.append(lax.all_gather(nw, "dp", axis=1, tiled=True))
            new_m.append(nm)
            new_v.append(nv)
        return (*new_w, *new_m, *new_v)

    whole, split = P(None, None, None), P(None, "dp", None)
    return jax.shard_map(
        step,
        mesh=mesh,
        in_specs=(P(("rep", "dp")),) * 2 + (whole,) * 3 + (split,) * 6,
        out_specs=(P("rep", None, None),) * 3 + (P("rep", "dp", None),) * 6,
        check_vma=False,
    )
```

```python
import functools

import jax
import jax.numpy as jnp
from jax import lax
from jax.experimental import pallas as pl
from jax.experimental.pallas import tpu as pltpu
from jax.sharding import PartitionSpec as P

F32, BF16 = jnp.float32, jnp.bfloat16
MESH = pl.DeviceIdType.MESH
EPS = 1e-6
VMEM_LIMIT = 67043328


def dot(a, b):
    return jnp.dot(a, b, preferred_element_type=F32)


def dot_nt(a, b):
    return lax.dot_general(a, b, (((1,), (1,)), ((), ())), preferred_element_type=F32)


def sigmoid(g):
    return 0.5 * jnp.tanh(0.5 * g) + 0.5


def scale_of(h):
    return lax.rsqrt(jnp.mean(h * h, -1, keepdims=True) + EPS)


def forward_kernel(z, x_ref, wg_ref, wu_ref, wd_ref, h1_ref, aT_ref, save_ref, a, wgu, wd, hid, *bufs):
    W, CH, NT, NC, T = z.W, z.CH, z.NT, z.NC, z.T
    gus, (wsem, dsem, osem) = bufs[:NC], bufs[NC:]

    def wcopy(t, slot):
        return (
            pltpu.make_async_copy(wg_ref.at[0, :, pl.ds(t * W, W)], wgu.at[slot, :, pl.ds(0, W)], wsem.at[slot, 0]),
            pltpu.make_async_copy(wu_ref.at[0, :, pl.ds(t * W, W)], wgu.at[slot, :, pl.ds(W, W)], wsem.at[slot, 1]),
        )

    for c in wcopy(0, 0):
        c.start()
    dcopy = pltpu.make_async_copy(wd_ref.at[0], wd, dsem)
    dcopy.start()
    for i in range(T // 256):
        r = pl.ds(i * 256, 256)
        h = x_ref[0, r, :].astype(F32)
        n = (h * scale_of(h)).astype(BF16)
        a[r, :] = n
        aT_ref[:, r] = n.T

    def out(t, c):
        return pltpu.make_async_copy(gus[c], save_ref.at[t, c], osem.at[c])

    def A(t, c):
        gu = dot(a[pl.ds(c * CH, CH), :], wgu[t % 2])
        gus[c][0] = gu[:, :W]
        gus[c][1] = gu[:, W:]

    def E(t, c):
        g, u = gus[c][0], gus[c][1]
        hid[pl.ds(c * CH, CH), pl.ds(pl.multiple_of(t * W, 128), W)] = (g * sigmoid(g) * u).astype(BF16)

    def tile(t, first):
        for c in wcopy(t, t % 2):
            c.wait()
        if first:
            for c in wcopy(t + 1, (t + 1) % 2):
                c.start()
        else:
            @pl.when(t + 1 < NT)
            def _():
                for c in wcopy(t + 1, (t + 1) % 2):
                    c.start()
        for p in range(0, NC, 2):
            if not first:
                out(t, p).wait()
                out(t, p + 1).wait()
            A(t, p)
            if p:
                E(t, p - 1)
            A(t, p + 1)
            E(t, p)
            if p:
                out(t, p - 2).start()
                out(t, p - 1).start()
        E(t, NC - 1)
        out(t, NC - 2).start()
        out(t, NC - 1).start()

    tile(0, True)

    @pl.loop(1, NT)
    def _(t):
        tile(t, False)

    dcopy.wait()

    @pl.loop(0, T // 512)
    def _(i):
        r = pl.ds(pl.multiple_of(i * 512, 512), 512)
        h1_ref[r, :] = x_ref[0, r, :] + dot(hid[r, :], wd[...]).astype(BF16)

    for c in range(NC):
        out(0, c).wait()


def backward_kernel(z, h1_ref, dy_ref, wg_ref, wu_ref, wd_ref, aT0_ref, save_ref,
                    gg_ref, gup_ref, gd_ref, fac_ref, dwd_ref,
                    a, aT, dyT, wgu, wd, gu0, gu1, gu2, gu3, dh0, dh1, hid, dgu, sd,
                    G, PB, OB, B1, B2, ssacc, ssall,
                    wsem, gsem, tsem, dsem, usem, sP, rP, sO, rO, s1, r1, s2, r2, sS, rS):
    W, CH, NT, NC, T, D = z.W, z.CH, z.NT, z.NC, z.T, z.D
    R = z.R
    NA, NB = 8, z.NS
    gus, dhs = (gu0, gu1, gu2, gu3), (dh0, dh1)
    da = None
    rep, me = lax.axis_index("rep"), lax.axis_index("dp")
    c, k = me // 2, me % 2
    partner = c * 2 + (1 - k)

    def dev(t):
        return (rep, t)

    def chip(j):
        return lax.rem(c + j + 4, 4)

    bar = pltpu.get_barrier_semaphore()
    for j in range(1, 8):
        pl.semaphore_signal(bar, inc=1, device_id=dev(lax.rem(me + j, 8)), device_id_type=MESH)

    def copyP(slot):
        return pltpu.make_async_remote_copy(src_ref=G.at[slot, :, 1 - k], dst_ref=PB.at[slot], send_sem=sP.at[slot], recv_sem=rP.at[slot],
                                            device_id=dev(partner), device_id_type=MESH)

    def copyO(slot, d):
        return pltpu.make_async_remote_copy(src_ref=G.at[slot, chip(2), k], dst_ref=OB.at[slot], send_sem=sO.at[slot], recv_sem=rO.at[slot],
                                            device_id=dev(chip(d) * 2 + k), device_id_type=MESH)

    def copy1(slot, d):
        return pltpu.make_async_remote_copy(src_ref=G.at[slot, chip(-d), k], dst_ref=B1.at[slot], send_sem=s1.at[slot], recv_sem=r1.at[slot],
                                            device_id=dev(chip(-d) * 2 + k), device_id_type=MESH)

    def copy2(slot, d):
        return pltpu.make_async_remote_copy(src_ref=G.at[slot, chip(d), k], dst_ref=B2.at[slot], send_sem=s2.at[slot], recv_sem=r2.at[slot],
                                            device_id=dev(chip(d) * 2 + k), device_id_type=MESH)

    def stage0(slot):
        copyP(slot).start()

    def stage1(slot, d):
        copyP(slot).wait_recv()
        for j, copy in ((2, copyO), (-d, copy1)):
            q = chip(j)
            G[slot, q, k] = (G[slot, q, k].astype(F32) + PB[slot, q].astype(F32)).astype(BF16)
            copy(slot, d).start()

    def stage2(slot, d):
        copyO(slot, d).wait_recv()
        q = chip(d)
        G[slot, q, k] = (G[slot, q, k].astype(F32) + PB[slot, q].astype(F32) + OB[slot].astype(F32)).astype(BF16)
        copy2(slot, d).start()

    def stage3(slot, d, put):
        copy1(slot, d).wait_recv()
        copy2(slot, d).wait_recv()
        s = (G[slot, c, k].astype(F32) + PB[slot, c].astype(F32)) + (B1[slot].astype(F32) + B2[slot].astype(F32))
        g = s.astype(BF16)
        put(g)
        w = g.astype(F32)
        ssacc[...] += jnp.sum((w * w).reshape(R // 8, 8, W), 0)
        copyP(slot).wait_send()
        copyO(slot, d).wait_send()
        copy1(slot, d).wait_send()
        copy2(slot, d).wait_send()

    def aslot(r, e):
        return lax.rem(r * 2 + e, NA)

    def when(p, f):
        if isinstance(p, bool):
            if p:
                f()
        else:
            pl.when(p)(f)

    DIR = (1, -1)

    def a_put(r, e):
        ref = (gg_ref, gup_ref)[e]
        layer = 1 - r // NT

        def put(g):
            ref[layer, :, pl.ds(pl.multiple_of(lax.rem(r, NT) * W, 128), W)] = g
        return put

    def round_a(r, s0=True, s1_=True, s2_=True, s3_=True):
        if s1_:
            def f1():
                for e in range(2):
                    stage1(aslot(r - 1, e), DIR[e])
            when(r >= 1 if not isinstance(r, int) else bool(r >= 1), f1)
        if s3_:
            def f3():
                for e in range(2):
                    stage3(aslot(r - 3, e), DIR[e], a_put(r - 3, e))
            when(r >= 3 if not isinstance(r, int) else bool(r >= 3), f3)
        if s2_:
            def f2():
                for e in range(2):
                    stage2(aslot(r - 2, e), DIR[e])
            when(r >= 2 if not isinstance(r, int) else bool(r >= 2), f2)
        if s0:
            for e in range(2):
                stage0(aslot(r, e))

    def bslot(i):
        return NA + i

    def bdir(layer, i):
        return 1 if (i + layer) % 2 else -1

    def b_load(layer, i):
        return pltpu.make_async_copy(dwd_ref.at[layer, :, :, i], G.at[bslot(i)], usem.at[i])

    def batch_b(layer, stage):
        for i in range(NB):
            if stage == 0:
                b_load(layer, i).wait()
                stage0(bslot(i))
            elif stage == 1:
                stage1(bslot(i), bdir(layer, i))
            elif stage == 2:
                stage2(bslot(i), bdir(layer, i))
            else:
                def put(g, i=i):
                    gd_ref[layer, pl.ds(i * R, R), :] = g
                stage3(bslot(i), bdir(layer, i), put)

    def wcopies(t, slot):
        return (
            pltpu.make_async_copy(wg_ref.at[1, :, pl.ds(t * W, W)], wgu.at[slot, :, pl.ds(0, W)], wsem.at[slot, 0]),
            pltpu.make_async_copy(wu_ref.at[1, :, pl.ds(t * W, W)], wgu.at[slot, :, pl.ds(W, W)], wsem.at[slot, 1]),
        )

    def dcopy(layer, t, slot):
        return pltpu.make_async_copy(wd_ref.at[layer, pl.ds(t * W, W), :], wd.at[slot], wsem.at[slot, 2])

    def sdcopy(layer, t, slot, b):
        B = t * 8 + b
        return pltpu.make_async_copy(sd.at[slot, pl.ds(b * R, R)], dwd_ref.at[layer, B // (2 * NB), lax.rem(B // NB, 2), lax.rem(B, NB)], dsem.at[slot, b])

    for cp in wcopies(0, 0) + (dcopy(1, 0, 0),):
        cp.start()
    hcopy = pltpu.make_async_copy(h1_ref, dgu.at[:, pl.ds(0, W)], tsem)
    hcopy.start()
    ssacc[...] = jnp.zeros_like(ssacc)
    hcopy.wait()

    @pl.loop(0, T // 128)
    def _(i):
        r = pl.ds(pl.multiple_of(i * 128, 128), 128)
        h = dgu[r, :W].astype(F32)
        n = (h * scale_of(h)).astype(BF16)
        a[r, :] = n
        aT[:, r] = n.T
        dyT[:, r] = dy_ref[0, r, :].T

    def da_at(ci):
        ref = gus[2 + ci // 2]
        return ref, ci % 2

    for ci in range(NC):
        ref, half = da_at(ci)
        ref[half] = jnp.zeros((CH, D), F32)

    pl.semaphore_wait(bar, 7)

    def back_elem(ci, gu, dh):
        r = pl.ds(ci * CH, CH)
        g, u, dh = gu[0], gu[1], dh[...].astype(F32)
        s = sigmoid(g)
        silu = g * s
        hid[r, :] = (silu * u).astype(BF16)
        dgu[r, :W] = (dh * u * (s + silu * (1.0 - s))).astype(BF16)
        dgu[r, W:] = (dh * silu).astype(BF16)

    def weight_grads(r, slot):
        for j in range(0, W, 256):
            n = min(256, W - j)
            sd[slot, j : j + n] = dot(dyT[...], hid[:, j : j + n]).astype(BF16).T
        for j in range(0, 2 * W, 256):
            gw = dot(aT[...], dgu[:, j : j + 256]).astype(BF16)
            for i in range(0, 256, 128):
                e, q = divmod(j + i, W)
                G[aslot(r, e), :, :, :, q : q + 128] = gw[:, i : i + 128].reshape(4, 2, R, 128)

    @pl.loop(0, NT)
    def _(t):
        slot = lax.rem(t, 2)
        for cp in wcopies(t, slot) + (dcopy(1, t, slot),):
            cp.wait()

        @pl.when(t + 1 < NT)
        def _():
            for cp in wcopies(t + 1, 1 - slot) + (dcopy(1, t + 1, 1 - slot),):
                cp.start()

        @pl.when(t >= 2)
        def _():
            for b in range(8):
                sdcopy(1, t - 2, slot, b).wait()

        def A(ci):
            r = pl.ds(ci * CH, CH)
            gu = dot(a[r, :], wgu[slot])
            gus[ci % 2][0] = gu[:, :W]
            gus[ci % 2][1] = gu[:, W:]
            dhs[ci % 2][...] = dot_nt(dy_ref[0, r, :], wd[slot]).astype(BF16)

        def DA(ci):
            ref, half = da_at(ci)
            ref[half] = ref[half] + dot_nt(dgu[pl.ds(ci * CH, CH), :], wgu[slot])

        for ci in range(NC):
            A(ci)
            if ci:
                back_elem(ci - 1, gus[(ci - 1) % 2], dhs[(ci - 1) % 2])
        for ci in range(NC - 1):
            DA(ci)
        back_elem(NC - 1, gus[(NC - 1) % 2], dhs[(NC - 1) % 2])
        weight_grads(t, slot)
        DA(NC - 1)
        for b in range(8):
            sdcopy(1, t, slot, b).start()
        round_a(t)

    hcopy.start()
    hcopy.wait()
    tcopy = pltpu.make_async_copy(aT0_ref, aT, tsem)
    tcopy.start()
    dcopy(0, 0, 0).start()

    def gcopy(t, ci):
        return pltpu.make_async_copy(save_ref.at[t, ci], gus[ci], gsem.at[ci])

    gcopy(0, 0).start()
    gcopy(0, 1).start()
    for ci in range(NC):
        ref, half = da_at(ci)
        @pl.loop(0, CH // 128)
        def _(j):
            r = pl.ds(pl.multiple_of(ci * CH + j * 128, 128), 128)
            h = dgu[r, :W].astype(F32)
            s = scale_of(h)
            d = ref[half, pl.ds(pl.multiple_of(j * 128, 128), 128), :].astype(BF16).astype(F32)
            kk = jnp.sum(d * h, -1, keepdims=True) * (s * s * s * (1.0 / D))
            n = dy_ref[0, r, :] + (d * s - h * kk).astype(BF16)
            a[r, :] = n
            dyT[:, r] = n.T
        if ci % 2:
            gcopy(0, 2 + ci // 2).start()
    for t in (NT - 2, NT - 1):
        for b in range(8):
            sdcopy(1, t, t % 2, b).wait()
    for i in range(NB):
        b_load(1, i).start()
    tcopy.wait()
    batch_b(1, 0)

    @pl.loop(0, NT)
    def _(t):
        slot = lax.rem(t, 2)
        dcopy(0, t, slot).wait()

        @pl.when(t + 1 < NT)
        def _():
            dcopy(0, t + 1, 1 - slot).start()

        @pl.when(t >= 2)
        def _():
            for b in range(8):
                sdcopy(0, t - 2, slot, b).wait()

        def A(ci):
            dhs[ci % 2][...] = dot_nt(a[pl.ds(ci * CH, CH), :], wd[slot]).astype(BF16)

        for ci in range(NC):
            A(ci)
            if ci:
                gcopy(t, ci - 1).wait()
                back_elem(ci - 1, gus[ci - 1], dhs[(ci - 1) % 2])
        gcopy(t, NC - 1).wait()
        back_elem(NC - 1, gus[NC - 1], dhs[(NC - 1) % 2])

        @pl.when(t + 1 < NT)
        def _():
            for ci in range(NC):
                gcopy(t + 1, ci).start()

        weight_grads(t + NT, slot)
        for b in range(8):
            sdcopy(0, t, slot, b).start()
        round_a(t + NT)
        for n in range(3):
            @pl.when(t == n)
            def _():
                batch_b(1, n + 1)

    for t in (NT - 2, NT - 1):
        for b in range(8):
            sdcopy(0, t, t % 2, b).wait()
    for i in range(NB):
        b_load(0, i).start()
    batch_b(0, 0)
    round_a(2 * NT, s0=False)
    batch_b(0, 1)
    round_a(2 * NT + 1, s0=False, s1_=False)
    batch_b(0, 2)
    round_a(2 * NT + 2, s0=False, s1_=False, s2_=False)
    batch_b(0, 3)

    acc = ssacc[...]
    part = acc[:, :128]
    for j in range(1, W // 128):
        part = part + acc[:, j * 128 : (j + 1) * 128]
    ssall[me] = part
    copies = []
    for j in range(1, 8):
        to = lax.rem(me + j, 8)
        cp = pltpu.make_async_remote_copy(src_ref=ssall.at[me], dst_ref=ssall.at[me], send_sem=sS.at[j - 1], recv_sem=rS.at[j - 1],
                                          device_id=dev(to), device_id_type=MESH)
        cp.start()
        copies.append(cp)
    for cp in copies:
        cp.wait()
    total = ssall[0]
    for j in range(1, 8):
        total = total + ssall[j]
    total = jnp.sum(jnp.sum(total, 0, keepdims=True), 1, keepdims=True)
    fac = jnp.minimum(1.0, 0.5 * lax.rsqrt(total / z.count + 1e-30))
    fac_ref[...] = jnp.broadcast_to(fac, fac_ref.shape)


class Sizes:
    pass


def solution(mesh):
    def step(x, dy, *arrays):
        weights, m, v = (arrays[i : i + 3] for i in (0, 3, 6))
        wg, wu, wd = weights
        z = Sizes()
        z.T, z.D = x.shape[1:]
        layers, _, z.FF = wg.shape
        z.W = z.D
        z.NT = z.FF // z.W
        z.CH = 512
        z.NC = z.T // z.CH
        z.R = z.D // 8
        z.NS = z.FF // 8 // z.R
        z.count = float(sum(w.size for w in weights))
        T, D, FF, W, CH, NT, NC, R, NS = z.T, z.D, z.FF, z.W, z.CH, z.NT, z.NC, z.R, z.NS
        vmem, hbm = pl.BlockSpec(memory_space=pltpu.VMEM), pl.BlockSpec(memory_space=pl.ANY)
        dma = pltpu.SemaphoreType.DMA
        h1, aT0, save = pl.pallas_call(
            functools.partial(forward_kernel, z),
            out_shape=(
                jax.ShapeDtypeStruct((T, D), BF16),
                jax.ShapeDtypeStruct((D, T), BF16),
                jax.ShapeDtypeStruct((NT, NC, 2, CH, W), F32),
            ),
            in_specs=[vmem] + [hbm] * 3,
            out_specs=(vmem, vmem, hbm),
            scratch_shapes=[
                pltpu.VMEM((T, D), BF16), pltpu.VMEM((2, D, 2 * W), BF16), pltpu.VMEM((FF, D), BF16), pltpu.VMEM((T, FF), BF16),
                *[pltpu.VMEM((2, CH, W), F32)] * NC,
                dma((2, 2)), dma, dma((NC,)),
            ],
            compiler_params=pltpu.CompilerParams(vmem_limit_bytes=VMEM_LIMIT),
            cost_estimate=pl.CostEstimate(flops=6 * T * D * FF, bytes_accessed=8 * T * FF, transcendentals=T * FF),
            name="forward0",
        )(x, wg, wu, wd)
        slots = 8 + NS
        block = pltpu.VMEM((slots, R, W), BF16)
        gg, gup, gd, fac, _ = pl.pallas_call(
            functools.partial(backward_kernel, z),
            out_shape=(
                jax.ShapeDtypeStruct((layers, R, FF), BF16),
                jax.ShapeDtypeStruct((layers, R, FF), BF16),
                jax.ShapeDtypeStruct((layers, NS * R, D), BF16),
                jax.ShapeDtypeStruct((8, 128), F32),
                jax.ShapeDtypeStruct((layers, 4, 2, NS, R, D), BF16),
            ),
            in_specs=[hbm, vmem] + [hbm] * 5,
            out_specs=(vmem, vmem, vmem, vmem, hbm),
            scratch_shapes=[
                pltpu.VMEM((T, D), BF16), pltpu.VMEM((D, T), BF16), pltpu.VMEM((D, T), BF16),
                pltpu.VMEM((2, D, 2 * W), BF16), pltpu.VMEM((2, W, D), BF16),
                *[pltpu.VMEM((2, CH, W), F32)] * NC,
                *[pltpu.VMEM((CH, W), BF16)] * 2,
                pltpu.VMEM((T, W), BF16), pltpu.VMEM((T, 2 * W), BF16), pltpu.VMEM((2, W, D), BF16),
                pltpu.VMEM((slots, 4, 2, R, W), BF16), pltpu.VMEM((slots, 4, R, W), BF16), block, block, block,
                pltpu.VMEM((8, W), F32), pltpu.VMEM((8, 8, 128), F32),
                dma((2, 3)), dma((NC,)), dma, dma((2, 8)), dma((NS,)),
                *[dma((slots,))] * 8, dma((7,)), dma((7,)),
            ],
            compiler_params=pltpu.CompilerParams(vmem_limit_bytes=VMEM_LIMIT, collective_id=0, has_side_effects=True),
            cost_estimate=pl.CostEstimate(flops=20 * T * D * FF, bytes_accessed=8 * T * FF, transcendentals=2 * T * FF),
            name="backward",
        )(h1, dy, wg, wu, wd, aT0, save)
        factor = fac[0, 0]
        me = lax.axis_index("dp")
        new_w, new_m, new_v = [], [], []
        for w, mm, vv, g in zip(weights, m, v, (gg, gup, gd), strict=True):
            rows = mm.shape[1]
            mine = lax.dynamic_slice_in_dim(w, me * rows, rows, 1).astype(F32)
            g = g.astype(F32) * factor
            nm = 0.9 * mm + 0.1 * g
            nv = 0.95 * vv + 0.05 * g * g
            nw = (mine - 0.02 * (nm * lax.rsqrt(nv + 1e-8) + 0.1 * mine)).astype(BF16)
            new_w.append(lax.all_gather(nw, "dp", axis=1, tiled=True))
            new_m.append(nm)
            new_v.append(nv)
        return (*new_w, *new_m, *new_v)

    whole, split = P(None, None, None), P(None, "dp", None)
    return jax.shard_map(
        step,
        mesh=mesh,
        in_specs=(P(("rep", "dp")),) * 2 + (whole,) * 3 + (split,) * 6,
        out_specs=(P("rep", None, None),) * 3 + (P("rep", "dp", None),) * 6,
        check_vma=False,
    )
```

```python
import functools
from types import SimpleNamespace

import jax
import jax.numpy as jnp
from jax import lax
from jax.experimental import pallas as pl
from jax.experimental.pallas import tpu as pltpu
from jax.sharding import PartitionSpec as P

F32, BF16 = jnp.float32, jnp.bfloat16
VMEM_LIMIT = 67043328
NT_DIMS = (((1,), (1,)), ((), ()))
copy = pltpu.make_async_copy


def dot(a, b):
    return jnp.dot(a, b, preferred_element_type=F32)


def dot_nt(a, b):
    return lax.dot_general(a, b, NT_DIMS, preferred_element_type=F32)


def sigmoid(g):
    return 0.5 * jnp.tanh(0.5 * g) + 0.5


def scale_of(h):
    return lax.rsqrt(jnp.mean(h * h, -1, keepdims=True) + 1e-6)


def span(i, n):
    return pl.ds(pl.multiple_of(i * n, n), n)


def start(*copies):
    for c in copies:
        c.start()


def wait(*copies):
    for c in copies:
        c.wait()


def gate_up_tiles(z, layer_of, wg_ref, wu_ref, wgu, sem):
    def copies(t):
        slot = lax.rem(t, 2)
        return [
            copy(ref.at[layer_of(t), :, span(lax.rem(t, z.NT), z.W)], wgu.at[slot, :, pl.ds(e * z.W, z.W)], sem.at[slot, e])
            for e, ref in enumerate((wg_ref, wu_ref))
        ]

    return copies


def forward_kernel(z, x_ref, dy_ref, wg_ref, wu_ref, wd_ref, h1_ref, a1_ref, a1T_ref, a0_ref, a0T_ref, dyT_ref, hid_ref,
                   a, a1, aT, cT, h1, dy, dyT, wgu, wd, hid, gu0, gu1, wsem, dsem, hsem, tsem):
    W, CH, NT, NC, T = z.W, z.CH, z.NT, z.NC, z.T
    gus = (gu0, gu1)
    tiles = gate_up_tiles(z, lambda t: 0, wg_ref, wu_ref, wgu, wsem)
    later = [copy(dy_ref.at[0], dy, dsem.at[0]), copy(wd_ref.at[0], wd, dsem.at[1])]
    start(*tiles(0), *later)
    step = CH // 2
    for i in range(T // step):
        r = pl.ds(i * step, step)
        h = x_ref[0, r, :].astype(F32)
        a[r, :] = (h * scale_of(h)).astype(BF16)
    pairs = (a, a0_ref), (aT, a0T_ref), (dyT, dyT_ref)
    whole = [copy(s, d, tsem.at[0, e]) for e, (s, d) in enumerate(pairs)]
    start(whole[0])
    wait(later[0])

    def hid_out(t):
        return copy(hid.at[:, span(t, W)], hid_ref.at[0, t], hsem.at[t])

    @pl.loop(0, NT)
    def _(t):
        wait(*tiles(t))

        @pl.when(t + 1 < NT)
        def _():
            start(*tiles(t + 1))

        turned = span(jnp.minimum(t, NC - 1), CH)
        aT[:, turned] = a[turned, :].T
        dyT[:, turned] = dy[turned, :].T

        def E(c):
            g, u = gus[c % 2][0], gus[c % 2][1]
            hid[pl.ds(c * CH, CH), span(t, W)] = (g * sigmoid(g) * u).astype(BF16)

        for c in range(NC):
            gu = dot(a[pl.ds(c * CH, CH), :], wgu[lax.rem(t, 2)])
            gus[c % 2][0] = gu[:, :W]
            gus[c % 2][1] = gu[:, W:]
            if c:
                E(c - 1)
        E(NC - 1)
        start(hid_out(t))

    start(*whole[1:])
    wait(later[1])

    def project(i):
        r = span(i, CH)
        h1[r, :] = x_ref[0, r, :] + dot(hid[r, :], wd[...]).astype(BF16)

    def norm(i):
        r = span(i, CH)
        h = h1[r, :].astype(F32)
        n = (h * scale_of(h)).astype(BF16)
        a1[r, :] = n
        cT[:, r] = n.T

    def done(i):
        r = span(i, CH)
        parts = (h1.at[r], h1_ref.at[r]), (a1.at[r], a1_ref.at[r]), (cT.at[:, r], a1T_ref.at[:, r])
        return [copy(s, d, tsem.at[1 + i, e]) for e, (s, d) in enumerate(parts)]

    project(0)

    @pl.loop(1, NC)
    def _(i):
        norm(i - 1)
        project(i)
        start(*done(i - 1))

    norm(NC - 1)
    start(*done(NC - 1))
    wait(*whole, *[d for i in range(NC) for d in done(i)], *[hid_out(t) for t in range(NT)])


def backward_kernel(z, h1_ref, a1_ref, a1T_ref, a0_ref, a0T_ref, dyT_ref, dy_ref, wg_ref, wu_ref, wd_ref,
                    mg_ref, vg_ref, mu_ref, vu_ref, md_ref, vd_ref, _,
                    gg_ref, gup_ref, gd_ref, fac_ref, nd_ref, og_ref, ou_ref, hid_ref,
                    a, aT, dy, dyT, wgu, wd, gu0, gu1, gu2, gu3, dh0, dh1, hids, dgu,
                    G, PB, OB, B1, B2, ssacc, ssall,
                    wsem, dsem, tsem, hsem, sP, rP, sO, rO, s1, r1, s2, r2, sS, rS,
                    msem, nsem, lsem, sR, rR, sL, rL, sX, rX, sD, rD):
    W, CH, NT, NC, D, R, NS = z.W, z.CH, z.NT, z.NC, z.D, z.R, z.NS
    NA = 6
    peers = 2 * z.chips
    gus, dhs = (gu0, gu1, gu2, gu3), (dh0, dh1)
    rep, me = lax.axis_index("rep"), lax.axis_index("dp")
    c, k = me // 2, lax.rem(me, 2)

    def chip(j):
        return lax.rem(c + j + z.chips, z.chips)

    def remote(src, dst, send, recv, to):
        return pltpu.make_async_remote_copy(src_ref=src, dst_ref=dst, send_sem=send, recv_sem=recv, device_id=(rep, to),
                                            device_id_type=pl.DeviceIdType.MESH)

    bar = pltpu.get_barrier_semaphore()
    for j in range(1, peers):
        pl.semaphore_signal(bar, inc=1, device_id=(rep, lax.rem(me + j, peers)), device_id_type=pl.DeviceIdType.MESH)

    partner = c * 2 + 1 - k

    def copyP(s):
        return remote(G.at[s, :, 1 - k], PB.at[s], sP.at[s], rP.at[s], partner)

    def copyO(s, d):
        return remote(G.at[s, chip(2), k], OB.at[s], sO.at[s], rO.at[s], chip(d) * 2 + k)

    def copy1(s, d):
        return remote(G.at[s, chip(-d), k], B1.at[s], s1.at[s], r1.at[s], chip(-d) * 2 + k)

    def copy2(s, d):
        return remote(G.at[s, chip(d), k], B2.at[s], s2.at[s], r2.at[s], chip(d) * 2 + k)

    def both(s, q):
        return G[s, q, k].astype(F32) + PB[s, q].astype(F32)

    def stage0(each):
        each(lambda s, d, put: copyP(s).start())

    def stage1(each):
        def add(s, d, put):
            for q in (chip(2), chip(-d)):
                G[s, q, k] = both(s, q).astype(BF16)

        each(lambda s, d, put: copyP(s).wait_recv())
        each(add)
        each(lambda s, d, put: copyO(s, d).start())
        each(lambda s, d, put: copy1(s, d).start())

    def stage2(each):
        def add(s, d, put):
            q = chip(d)
            G[s, q, k] = (both(s, q) + OB[s].astype(F32)).astype(BF16)

        each(lambda s, d, put: copyO(s, d).wait_recv())
        each(add)
        each(lambda s, d, put: copy2(s, d).start())

    def stage3(each):
        def arrive(s, d, put):
            copy1(s, d).wait_recv()
            copy2(s, d).wait_recv()

        def add(s, d, put):
            g = (both(s, c) + (B1[s].astype(F32) + B2[s].astype(F32))).astype(BF16)
            put(g)
            w = g.astype(F32)
            ssacc[...] += jnp.sum((w * w).reshape(-1, *ssacc.shape), 0)

        def sent(s, d, put):
            for cp in (copyP(s), copyO(s, d), copy1(s, d), copy2(s, d)):
                cp.wait_send()

        for f in (arrive, add, sent):
            each(f)

    stages = stage0, stage1, stage2, stage3

    def a_slot(r, e):
        return lax.rem(r * 2 + e, NA)

    def a_put(r, e):
        def put(g):
            (gg_ref, gup_ref)[e][1 - r // NT, :, span(lax.rem(r, NT), W)] = g

        return put

    def stream_a(stage, r):
        stages[stage](lambda f: [f(a_slot(r, e), d, a_put(r, e)) for e, d in enumerate((1, -1))])

    def stream_b(stage, layer):
        def put(i):
            def f(g):
                gd_ref[layer, span(i, R), :] = g

            return f

        stages[stage](lambda f: pl.loop(0, NS)(lambda i: f(NA + i, lax.rem(i + layer, 2) * 2 - 1, put(i))))

    def layer_of(r):
        return 1 - r // NT

    tiles = gate_up_tiles(z, layer_of, wg_ref, wu_ref, wgu, wsem)

    def down(r):
        slot = lax.rem(r, 2)
        return copy(wd_ref.at[layer_of(r), span(lax.rem(r, NT), W), :], wd.at[slot], dsem.at[slot])

    def hid_out(t):
        return copy(hids.at[0], hid_ref.at[1, t], hsem.at[0])

    def gate_up_grads(r):
        for j in range(0, 2 * W, 256):
            gw = dot(aT[...], dgu[:, j : j + 256]).astype(BF16)
            for i in range(0, 256, 128):
                e, q = divmod(j + i, W)
                G[a_slot(r, e), :, :, :, q : q + 128] = gw[:, i : i + 128].reshape(*G.shape[1:4], 128)

    def hid_in(layer, i):
        return copy(hid_ref.at[layer, NT - 1 - i], hids.at[lax.rem(i, 2)], hsem.at[lax.rem(i, 2)])

    def turn_units(sd, i):
        for j in range(0, W, 128):
            rows = sd[:, j : j + 128].T
            for b in range(8):
                lo, hi = max(j, b * R), min(j + 128, b * R + R)
                if lo < hi:
                    B = (NT - 1 - i) * 8 + b
                    unit = G.at[NA + lax.rem(B, NS), B // (2 * NS), lax.rem(B // NS, 2)]
                    unit[lo - b * R : hi - b * R] = rows[lo - j : hi - j]

    def down_grads(layer, sd):
        @pl.loop(0, NT)
        def _(i):
            slot = lax.rem(i, 2)

            @pl.when(i + 1 > layer)
            def _():
                wait(hid_in(layer, i))

            turn_units(sd, jnp.maximum(i - 1, 0))
            for j in range(0, W, 256):
                n = min(256, W - j)
                sd[:, j : j + n] = dot(dyT[...], hids[slot, :, j : j + n]).astype(BF16)

            @pl.when(i + 2 < NT)
            def _():
                start(hid_in(layer, i + 2))

            @pl.when((i == 1) & (layer == 1))
            def _():
                stream_a(1, NT - 1)
                stream_a(3, NT - 2)

        turn_units(sd, NT - 1)

    def da_at(ci):
        return (gu2, gu3)[ci // 2].at[ci % 2]

    def output_grad(ci):
        step = CH // 2

        @pl.loop(0, 2)
        def _(j):
            r = span(ci * 2 + j, step)
            h = dgu[r, :W].astype(F32)
            s = scale_of(h)
            d = da_at(ci)[span(j, step), :].astype(BF16).astype(F32)
            n = dy[r, :] + (s * (d - h * (s * s * jnp.mean(d * h, -1, keepdims=True)))).astype(BF16)
            dy[r, :] = n
            dyT[:, r] = n.T

    swap = [copy(s, d, tsem.at[i]) for i, (s, d) in enumerate(((h1_ref, dgu.at[:, pl.ds(0, W)]), (a0_ref, a), (a0T_ref, aT)))]

    def turn():
        wait(*swap)
        output_grad(0)
        output_grad(1)
        output_grad(2)
        output_grad(3)
        stream_a(2, NT - 1)
        stream_b(1, 1)

    first = [copy(a1_ref, a, tsem.at[0]), copy(dy_ref.at[0], dy, tsem.at[1]), copy(a1T_ref, aT, tsem.at[2]), copy(dyT_ref, dyT, tsem.at[3])]
    start(first[0], *tiles(0), down(0), *first[1:])
    ssacc[...] = jnp.zeros_like(ssacc)
    for ci in range(NC):
        da_at(ci)[...] = jnp.zeros((CH, D), F32)
    pl.semaphore_wait(bar, peers - 1)
    wait(*first[:2])

    @pl.loop(0, 2 * NT)
    def _(r):
        slot = lax.rem(r, 2)

        @pl.when((r == NT) | (r == NT + 2))
        def _():
            layer = 1 - (r - NT) // 2
            down_grads(layer, wd.at[1 - slot])

            @pl.when(layer == 1)
            def _():
                stream_b(0, 1)


        pl.when(r == NT)(turn)
        wait(*tiles(r), down(r))

        @pl.when(r + 1 < 2 * NT)
        def _():
            start(*tiles(r + 1), down(r + 1))

        @pl.when((r >= 1) & (r < NT))
        def _():
            wait(hid_out(r - 1))

        def A(ci):
            rows = pl.ds(ci * CH, CH)
            gu = dot(a[rows, :], wgu[slot])
            gus[ci % 2][0] = gu[:, :W]
            gus[ci % 2][1] = gu[:, W:]
            dhs[ci % 2][...] = dot_nt(dy[rows, :], wd[slot]).astype(BF16)

        def E(ci):
            rows = pl.ds(ci * CH, CH)
            gu = gus[ci % 2]
            g, u, d = gu[0], gu[1], dhs[ci % 2][...].astype(F32)
            s = sigmoid(g)
            silu = g * s
            hids[0, rows, :] = (silu * u).astype(BF16)
            dgu[rows, :W] = (d * u * (s + silu * (1.0 - s))).astype(BF16)
            dgu[rows, W:] = (d * silu).astype(BF16)

        for ci in range(NC):
            A(ci)
            if ci:
                E(ci - 1)
        E(NC - 1)

        @pl.when(r < NT - 1)
        def _():
            start(hid_out(r))

        @pl.when((r >= 1) & (r != NT))
        def _():
            stream_a(1, r - 1)

            @pl.when(r >= 2)
            def _():
                stream_a(3, r - 2)

            @pl.when(r == NT + 1)
            def _():
                stream_b(3, 1)

            @pl.when(r == NT + 2)
            def _():
                stream_b(0, 0)

        @pl.when(r == 0)
        def _():
            wait(*first[2:])

        gate_up_grads(r)
        stream_a(0, r)

        @pl.when(r < NT)
        def _():
            @pl.loop(0, 2)
            def _(half):
                for i, ref in enumerate((gu2, gu3)):
                    ref[half] += dot_nt(dgu[span(i * 2 + half, CH), :], wgu[slot])

            @pl.when(r == NT - 1)
            def _():
                start(*swap, hid_in(1, 1))

        @pl.when((r >= 1) & (r != NT))
        def _():
            stream_a(2, r - 1)

        @pl.when(r >= NT)
        def _():
            @pl.when(r == NT)
            def _():
                stream_b(2, 1)

            @pl.when(r == NT + 1)
            def _():
                start(hid_in(0, 0), hid_in(0, 1))

            @pl.when(r == NT + 2)
            def _():
                stream_b(1, 0)

            @pl.when(r == NT + 3)
            def _():
                stream_b(2, 0)

    R2 = NS * R

    def block(ref, i, layer, t):
        return ref.at[layer, span(i, R), span(t, W)]

    def nw(e, layer, t):
        return hids.at[e, span(layer * NT + t, R)]

    @pl.loop(0, NT)
    def _(t):
        for layer in range(2):
            for i, ref in enumerate((mg_ref, vg_ref, mu_ref, vu_ref)):
                start(copy(block(ref, 0, layer, t), gus[i].at[layer, span(t, R)], msem.at[i]))
            for e, ref in enumerate((wg_ref, wu_ref)):
                start(copy(block(ref, me, layer, t), nw(e, layer, t), nsem.at[e]))

    def arrived(ref, sem):
        wait(copy(ref, ref, sem))

    own_down = [copy(wd_ref.at[layer, span(me, R2), :], a.at[pl.ds(layer * R2, R2)], nsem.at[2 + layer]) for layer in range(2)]
    start(*own_down)

    last = 2 * NT - 1
    stream_a(1, last)
    stream_a(3, last - 1)
    stream_a(2, last)
    stream_b(3, 0)
    stream_a(3, last)

    lanes = ssall.shape[-1]
    part = ssacc[:, :lanes]
    for j in range(1, W // lanes):
        part = part + ssacc[:, j * lanes : (j + 1) * lanes]
    ssall[me] = part
    parts = [remote(ssall.at[me], ssall.at[me], sS.at[j], rS.at[j], lax.rem(me + j, peers)) for j in range(1, peers)]
    start(*parts)
    wait(*parts)
    total = ssall[0]
    for j in range(1, peers):
        total = total + ssall[j]
    total = jnp.sum(jnp.sum(total, 0, keepdims=True), 1, keepdims=True)
    fac = jnp.minimum(1.0, 0.5 * lax.rsqrt(total / z.count + 1e-30))
    fac_ref[...] = jnp.broadcast_to(fac, fac_ref.shape)

    def new_weight(w, m, v, g):
        w, g = w.astype(F32), g.astype(F32) * fac
        m = 0.9 * m + 0.1 * g
        v = 0.95 * v + 0.05 * g * g
        return (w - 0.02 * (m * lax.rsqrt(v + 1e-8) + 0.1 * w)).astype(BF16)

    outs = (og_ref, ou_ref)
    chunks = [(e, layer) for e in range(2) for layer in range(2)]

    def here(q, j):
        e, layer = chunks[q]
        return outs[e].at[layer, span(chip(j) * 2 + k, R)]

    def send(q, j, send, recv, to):
        return remote(here(q, j), here(q, j), send, recv, to)

    def right_of(q):
        return send(q, 0, sR.at[q], rR.at[q], chip(1) * 2 + k)

    def left_of(q):
        return send(q, 0, sL.at[q], rL.at[q], chip(-1) * 2 + k)

    def across(q):
        j = chunks[q][0] * 2 - 1
        return send(q, j, sX.at[q], rX.at[q], chip(-j) * 2 + k)

    def over(q, i):
        return send(q, (0, -1, 1, 2)[i], sD.at[q, i], rD.at[q, i], partner)

    def leave(q):
        arrived(here(q, 0), lsem.at[q])
        start(right_of(q), left_of(q), over(q, 0))

    for q, (e, layer) in enumerate(chunks):
        if layer == 0:
            arrived(hids.at[e, pl.ds(0, 2 * NT * R)], nsem.at[e])
            for i in (2 * e, 2 * e + 1):
                arrived(gus[i].at[:, pl.ds(0, NT * R)], msem.at[i])

        @pl.loop(0, NT)
        def _(t):
            held = span(t, R)
            own = nw(e, layer, t)
            own[...] = new_weight(own[...], gus[2 * e][layer, held], gus[2 * e + 1][layer, held], (gg_ref, gup_ref)[e][layer, :, span(t, W)])
            start(copy(own, block(outs[e], me, layer, t), lsem.at[q]))

        if q:
            leave(q - 1)
    leave(len(chunks) - 1)
    moments = [copy(ref, gus[i].at[:, pl.ds(0, R2)], msem.at[i]) for i, ref in enumerate((md_ref, vd_ref))]
    start(*moments)
    wait(*own_down, *moments)

    @pl.loop(0, NS)
    def _(i):
        for layer in range(2):
            held, own = span(i, R), span(layer * NS + i, R)
            a[own, :] = new_weight(a[own, :], gus[0][layer, held], gus[1][layer, held], gd_ref[layer, held])

    new_down = [copy(a.at[pl.ds(layer * R2, R2)], nd_ref.at[layer], nsem.at[2 + layer]) for layer in range(2)]
    start(*new_down)
    for q, (e, layer) in enumerate(chunks):
        right_of(q).wait_recv()
        if e == 0:
            start(across(q))
        start(over(q, 1))
        left_of(q).wait_recv()
        if e:
            start(across(q))
        start(over(q, 2))
    for q in range(len(chunks)):
        across(q).wait_recv()
        start(over(q, 3))
    wait(*new_down)
    for q in range(len(chunks)):
        wait(*[over(q, i) for i in range(4)])
        for sent in (right_of(q), left_of(q), across(q)):
            sent.wait_send()


def copy_kernel(og_ref, ou_ref, ng_ref, nu_ref, buf, isem, osem):
    n, rows = buf.shape[:2]
    per = n // 2
    ins, outs = [], []
    for i in range(n):
        src, dst = ((og_ref, ng_ref), (ou_ref, nu_ref))[i // per]
        at = pl.ds(i % per * rows, rows)
        ins.append(copy(src.at[at], buf.at[i], isem.at[i]))
        outs.append(copy(buf.at[i], dst.at[at], osem.at[i]))
    start(*ins)
    for i in range(n):
        wait(ins[i])
        start(outs[i])
    wait(*outs)


def moments_kernel(fac_ref, *refs):
    ins, outs = refs[:9], refs[9:]
    for i in range(3):
        m, v, g = (r[0] for r in ins[3 * i : 3 * i + 3])
        g = g.astype(F32) * fac_ref[:1, :1]
        outs[2 * i][0] = 0.9 * m + 0.1 * g
        outs[2 * i + 1][0] = 0.95 * v + 0.05 * g * g


def place_kernel(firsts, at_ref, *refs):
    out, sem = refs[-2:]
    copies = []
    for i, first in enumerate(firsts):
        count, rows = refs[i].shape[:2]
        copies.append(copy(refs[i], out.at[pl.ds(first, count), pl.ds(pl.multiple_of(at_ref[i] * rows, 16), rows)], sem.at[i]))
    start(*copies)
    wait(*copies)


VMEM, HBM = pl.BlockSpec(memory_space=pltpu.VMEM), pl.BlockSpec(memory_space=pl.ANY)
dma = pltpu.SemaphoreType.DMA


def bf16(*shape):
    return pltpu.VMEM(shape, BF16)


def f32(*shape):
    return pltpu.VMEM(shape, F32)


def call(kernel, ins, out, scratch, cost, limit=VMEM_LIMIT, **params):
    flops, moved = cost
    more = {key: params.pop(key) for key in ("grid", "input_output_aliases") if key in params}
    outs = [spec for _, _, spec in out]
    shapes = [jax.ShapeDtypeStruct(shape, dtype) for shape, dtype, _ in out]
    return pl.pallas_call(
        kernel,
        out_shape=shapes,
        in_specs=ins,
        out_specs=outs,
        scratch_shapes=scratch,
        compiler_params=pltpu.CompilerParams(vmem_limit_bytes=limit, **params),
        cost_estimate=pl.CostEstimate(flops=int(flops), bytes_accessed=int(moved), transcendentals=0),
        **more,
    )


def solution(mesh):
    n = mesh.shape["dp"]
    chips = n // 2

    def ring(shift, flip=0):
        return [(i, (i // 2 + shift) % chips * 2 + (i + flip) % 2) for i in range(n)]

    def right(t):
        return lax.ppermute(t, "dp", ring(1))

    def left(t):
        return lax.ppermute(t, "dp", ring(-1))

    def partner(t):
        return lax.ppermute(t, "dp", ring(0, 1))

    def step(x, dy, *arrays):
        weights, m, v = (arrays[i : i + 3] for i in (0, 3, 6))
        wg, wu, wd = weights
        T, D = x.shape[1:]
        layers, _, FF = wg.shape
        W, CH = D, 512
        NT, NC, R = FF // W, T // CH, D // n
        NS = FF // n // R
        z = SimpleNamespace(T=T, D=D, FF=FF, W=W, CH=CH, NT=NT, NC=NC, R=R, NS=NS, chips=chips, count=float(sum(w.size for w in weights)))
        tokens, turned, hidden = ((T, D), BF16, HBM), ((D, T), BF16, HBM), ((layers, NT, T, W), BF16, HBM)
        h1, a1, a1T, a0, a0T, dyT, hid = call(
            functools.partial(forward_kernel, z), [VMEM] + [HBM] * 4,
            [tokens, tokens, turned, tokens, turned, turned, hidden],
            [*[bf16(T, D)] * 2, *[bf16(D, T)] * 2, *[bf16(T, D)] * 2, bf16(D, T), bf16(2, D, 2 * W), bf16(FF, D), bf16(T, FF), *[f32(2, CH, W)] * 2,
             dma((2, 2)), dma((2,)), dma((NT,)), dma((NC + 1, 3))],
            (6 * T * D * FF, 8 * T * FF),
        )(x, dy, wg, wu, wd)
        slots = 6 + NS
        blocks = bf16(slots, R, W)
        flat, tall, gathered = (layers, R, FF), (layers, NS * R, D), (layers, D, FF)
        gg, gup, gd, fac, nd, og, ou, _ = call(
            functools.partial(backward_kernel, z), [HBM] * 17,
            [(flat, BF16, VMEM), (flat, BF16, VMEM), (tall, BF16, VMEM), ((8, 128), F32, VMEM), (tall, BF16, HBM),
             (gathered, BF16, HBM), (gathered, BF16, HBM), hidden],
            [bf16(T, D), bf16(D, T), bf16(T, D), bf16(D, T), bf16(2, D, 2 * W), bf16(2, W, D), *[f32(2, CH, W)] * 4, *[bf16(CH, W)] * 2,
             bf16(2, T, W), bf16(T, 2 * W),
             bf16(slots, chips, 2, R, W), bf16(slots, chips, R, W), blocks, blocks, blocks, f32(8, W), f32(n, 8, 128),
             dma((2, 2)), dma((2,)), dma((4,)), dma((2,)), *[dma((slots,))] * 8, dma((n,)), dma((n,)),
             *[dma((4,))] * 9, *[dma((4, 4))] * 2],
            (24 * T * D * FF, 8 * T * FF), collective_id=0, has_side_effects=True, input_output_aliases={16: 7},
        )(h1, a1, a1T, a0, a0T, dyT, dy, wg, wu, wd, m[0], v[0], m[1], v[1], m[2], v[2], hid)

        me = lax.axis_index("dp")
        c, k = me // 2, lax.rem(me, 2)

        def place(out, pieces):
            ts = [t for t, _, _ in pieces]
            count = len(ts)
            known = () if out is None else (out,)
            return call(
                functools.partial(place_kernel, [first for _, _, first in pieces]),
                [pl.BlockSpec(memory_space=pltpu.SMEM)] + [VMEM] * count + [HBM] * len(known), [(wd.shape, BF16, HBM)], [dma((count,))],
                (2e6 * count, 4 * sum(t.size for t in ts)), 1 << 24, input_output_aliases={count + 1: 0} if known else {},
            )(jnp.stack([at for _, at, _ in pieces]).astype(jnp.int32), *ts, *known)[0]

        def spot(shift, core):
            return lax.rem(c + shift + chips, chips) * 2 + core

        from_left, from_right = right(nd), left(nd)
        p_own = partner(nd)
        rows = layers * D
        parts = [(rows, FF), BF16, HBM]
        ng, nu = call(
            copy_kernel, [HBM] * 2, [parts] * 2, [bf16(8, rows // 4, FF), dma((8,)), dma((8,))], (12e9, 8 * rows * FF),
        )(og.reshape(rows, FF), ou.reshape(rows, FF))
        wide = pl.BlockSpec((1, R, W), lambda i, j: (i, 0, j))
        high = pl.BlockSpec((1, R, W), lambda i, j: (i, j, 0))
        kinds = ((flat, wide), (flat, wide), (tall, high))
        moved = call(
            moments_kernel, [pl.BlockSpec((8, 128), lambda i, j: (0, 0))] + [spec for _, spec in kinds for _ in range(3)],
            [(shape, F32, spec) for shape, spec in kinds for _ in range(2)], [], (10e9, 54 * m[0].size), grid=(layers, NT),
        )(fac, *[t for i, g in enumerate((gg, gup, gd)) for t in (m[i], v[i], g)])
        opp = right(from_left[:1]), left(from_right[1:])
        p_left, p_right = partner(from_left), partner(from_right)
        sides = ((nd, p_own, 0), (from_left, p_left, -1), (from_right, p_right, 1))
        out = place(None, [piece for t, p, j in sides for piece in ((t, spot(j, k), 0), (p, spot(j, 1 - k), 0))])
        p_opp = [partner(t) for t in opp]
        out = place(out, [piece for i in range(2) for piece in ((opp[i], spot(2, k), i), (p_opp[i], spot(2, 1 - k), i))])
        return ng.reshape(gathered), nu.reshape(gathered), out, *moved[::2], *moved[1::2]

    whole, split = P(None, None, None), P(None, "dp", None)
    step = jax.shard_map(
        step,
        mesh=mesh,
        in_specs=(P(("rep", "dp")),) * 2 + (whole,) * 3 + (split,) * 6,
        out_specs=(P("rep", None, None),) * 3 + (P("rep", "dp", None),) * 6,
        check_vma=False,
    )
    return step
```

```python
import functools
from types import SimpleNamespace

import jax
import jax.numpy as jnp
from jax import lax
from jax.experimental import pallas as pl
from jax.experimental.pallas import tpu as pltpu
from jax.sharding import PartitionSpec as P

F32, BF16 = jnp.float32, jnp.bfloat16
VMEM_LIMIT = 67043328
NT_DIMS = (((1,), (1,)), ((), ()))
copy = pltpu.make_async_copy


def dot(a, b):
    return jnp.dot(a, b, preferred_element_type=F32)


def dot_nt(a, b):
    return lax.dot_general(a, b, NT_DIMS, preferred_element_type=F32)


def sigmoid(g):
    return 0.5 * jnp.tanh(0.5 * g) + 0.5


def scale_of(h):
    return lax.rsqrt(jnp.mean(h * h, -1, keepdims=True) + 1e-6)


def span(i, n):
    return pl.ds(pl.multiple_of(i * n, n), n)


def start(*copies):
    for c in copies:
        c.start()


def wait(*copies):
    for c in copies:
        c.wait()


def gate_up_tiles(z, layer_of, wg_ref, wu_ref, wgu, sem):
    def copies(t):
        slot = lax.rem(t, 2)
        return [
            copy(ref.at[layer_of(t), :, span(lax.rem(t, z.NT), z.W)], wgu.at[slot, :, pl.ds(e * z.W, z.W)], sem.at[slot, e])
            for e, ref in enumerate((wg_ref, wu_ref))
        ]

    return copies


def forward_kernel(z, x_ref, dy_ref, wg_ref, wu_ref, wd_ref, h1_ref, a1_ref, a1T_ref, a0_ref, a0T_ref, dyT_ref, hid_ref,
                   a, a1, aT, cT, h1, dy, dyT, wgu, wd, hid, gu0, gu1, wsem, dsem, hsem, tsem):
    W, CH, NT, NC, T = z.W, z.CH, z.NT, z.NC, z.T
    gus = (gu0, gu1)
    tiles = gate_up_tiles(z, lambda t: 0, wg_ref, wu_ref, wgu, wsem)
    later = [copy(dy_ref.at[0], dy, dsem.at[0]), copy(wd_ref.at[0], wd, dsem.at[1])]
    start(*tiles(0), *later)
    step = CH // 2
    for i in range(T // step):
        r = pl.ds(i * step, step)
        h = x_ref[0, r, :].astype(F32)
        a[r, :] = (h * scale_of(h)).astype(BF16)
    pairs = (a, a0_ref), (aT, a0T_ref), (dyT, dyT_ref)
    whole = [copy(s, d, tsem.at[0, e]) for e, (s, d) in enumerate(pairs)]
    start(whole[0])
    wait(later[0])

    def hid_out(t):
        return copy(hid.at[:, span(t, W)], hid_ref.at[0, t], hsem.at[t])

    @pl.loop(0, NT)
    def _(t):
        wait(*tiles(t))

        @pl.when(t + 1 < NT)
        def _():
            start(*tiles(t + 1))

        turned = span(jnp.minimum(t, NC - 1), CH)
        aT[:, turned] = a[turned, :].T
        dyT[:, turned] = dy[turned, :].T

        def E(c):
            g, u = gus[c % 2][0], gus[c % 2][1]
            hid[pl.ds(c * CH, CH), span(t, W)] = (g * sigmoid(g) * u).astype(BF16)

        for c in range(NC):
            gu = dot(a[pl.ds(c * CH, CH), :], wgu[lax.rem(t, 2)])
            gus[c % 2][0] = gu[:, :W]
            gus[c % 2][1] = gu[:, W:]
            if c:
                E(c - 1)
        E(NC - 1)
        start(hid_out(t))

    start(*whole[1:])
    wait(later[1])

    def project(i):
        r = span(i, CH)
        h1[r, :] = x_ref[0, r, :] + dot(hid[r, :], wd[...]).astype(BF16)

    def norm(i):
        r = span(i, CH)
        h = h1[r, :].astype(F32)
        n = (h * scale_of(h)).astype(BF16)
        a1[r, :] = n
        cT[:, r] = n.T

    def done(i):
        r = span(i, CH)
        parts = (h1.at[r], h1_ref.at[r]), (a1.at[r], a1_ref.at[r]), (cT.at[:, r], a1T_ref.at[:, r])
        return [copy(s, d, tsem.at[1 + i, e]) for e, (s, d) in enumerate(parts)]

    project(0)

    @pl.loop(1, NC)
    def _(i):
        norm(i - 1)
        project(i)
        start(*done(i - 1))

    norm(NC - 1)
    start(*done(NC - 1))
    wait(*whole, *[d for i in range(NC) for d in done(i)], *[hid_out(t) for t in range(NT)])


def backward_kernel(z, h1_ref, a1_ref, a1T_ref, a0_ref, a0T_ref, dyT_ref, dy_ref, wg_ref, wu_ref, wd_ref,
                    mg_ref, vg_ref, mu_ref, vu_ref, md_ref, vd_ref, _,
                    gg_ref, gup_ref, gd_ref, fac_ref, nd_ref, n0_ref, n1_ref, og_ref, ou_ref, hid_ref,
                    a, aT, dy, dyT, wgu, wd, gu0, gu1, gu2, gu3, dh0, dh1, hids, dgu,
                    G, PB, OB, B1, B2, ssacc, ssall,
                    wsem, dsem, tsem, hsem, sP, rP, sO, rO, s1, r1, s2, r2, sS, rS,
                    msem, nsem, lsem, sR, rR, sL, rL, sX, rX, sD, rD):
    W, CH, NT, NC, D, R, NS = z.W, z.CH, z.NT, z.NC, z.D, z.R, z.NS
    NA = 6
    peers = 2 * z.chips
    gus, dhs = (gu0, gu1, gu2, gu3), (dh0, dh1)
    rep, me = lax.axis_index("rep"), lax.axis_index("dp")
    c, k = me // 2, lax.rem(me, 2)

    def chip(j):
        return lax.rem(c + j + z.chips, z.chips)

    def remote(src, dst, send, recv, to):
        return pltpu.make_async_remote_copy(src_ref=src, dst_ref=dst, send_sem=send, recv_sem=recv, device_id=(rep, to),
                                            device_id_type=pl.DeviceIdType.MESH)

    bar = pltpu.get_barrier_semaphore()
    for j in range(1, peers):
        pl.semaphore_signal(bar, inc=1, device_id=(rep, lax.rem(me + j, peers)), device_id_type=pl.DeviceIdType.MESH)

    partner = c * 2 + 1 - k

    def copyP(s):
        return remote(G.at[s, :, 1 - k], PB.at[s], sP.at[s], rP.at[s], partner)

    def copyO(s, d):
        return remote(G.at[s, chip(2), k], OB.at[s], sO.at[s], rO.at[s], chip(d) * 2 + k)

    def copy1(s, d):
        return remote(G.at[s, chip(-d), k], B1.at[s], s1.at[s], r1.at[s], chip(-d) * 2 + k)

    def copy2(s, d):
        return remote(G.at[s, chip(d), k], B2.at[s], s2.at[s], r2.at[s], chip(d) * 2 + k)

    def both(s, q):
        return G[s, q, k].astype(F32) + PB[s, q].astype(F32)

    def stage0(each):
        each(lambda s, d, put: copyP(s).start())

    def stage1(each):
        def add(s, d, put):
            for q in (chip(2), chip(-d)):
                G[s, q, k] = both(s, q).astype(BF16)

        each(lambda s, d, put: copyP(s).wait_recv())
        each(add)
        each(lambda s, d, put: copyO(s, d).start())
        each(lambda s, d, put: copy1(s, d).start())

    def stage2(each):
        def add(s, d, put):
            q = chip(d)
            G[s, q, k] = (both(s, q) + OB[s].astype(F32)).astype(BF16)

        each(lambda s, d, put: copyO(s, d).wait_recv())
        each(add)
        each(lambda s, d, put: copy2(s, d).start())

    def stage3(each):
        def arrive(s, d, put):
            copy1(s, d).wait_recv()
            copy2(s, d).wait_recv()

        def add(s, d, put):
            g = (both(s, c) + (B1[s].astype(F32) + B2[s].astype(F32))).astype(BF16)
            put(g)
            w = g.astype(F32)
            ssacc[...] += jnp.sum((w * w).reshape(-1, *ssacc.shape), 0)

        def sent(s, d, put):
            for cp in (copyP(s), copyO(s, d), copy1(s, d), copy2(s, d)):
                cp.wait_send()

        for f in (arrive, add, sent):
            each(f)

    stages = stage0, stage1, stage2, stage3

    def a_slot(r, e):
        return lax.rem(r * 2 + e, NA)

    def a_put(r, e):
        def put(g):
            (gg_ref, gup_ref)[e][1 - r // NT, :, span(lax.rem(r, NT), W)] = g

        return put

    def stream_a(stage, r):
        stages[stage](lambda f: [f(a_slot(r, e), d, a_put(r, e)) for e, d in enumerate((1, -1))])

    def stream_b(stage, layer):
        def put(i):
            def f(g):
                gd_ref[layer, span(i, R), :] = g

            return f

        stages[stage](lambda f: pl.loop(0, NS)(lambda i: f(NA + i, lax.rem(i + layer, 2) * 2 - 1, put(i))))

    def layer_of(r):
        return 1 - r // NT

    tiles = gate_up_tiles(z, layer_of, wg_ref, wu_ref, wgu, wsem)

    def down(r):
        slot = lax.rem(r, 2)
        return copy(wd_ref.at[layer_of(r), span(lax.rem(r, NT), W), :], wd.at[slot], dsem.at[slot])

    def hid_out(t):
        return copy(hids.at[0], hid_ref.at[1, t], hsem.at[0])

    def gate_up_grads(r):
        for j in range(0, 2 * W, 256):
            gw = dot(aT[...], dgu[:, j : j + 256]).astype(BF16)
            for i in range(0, 256, 128):
                e, q = divmod(j + i, W)
                G[a_slot(r, e), :, :, :, q : q + 128] = gw[:, i : i + 128].reshape(*G.shape[1:4], 128)

    def hid_in(layer, i, slot):
        return copy(hid_ref.at[layer, NT - 1 - i], hids.at[lax.rem(slot, 2)], hsem.at[lax.rem(slot, 2)])

    def turn_units(sd, i):
        for j in range(0, W, 128):
            rows = sd[:, j : j + 128].T
            for b in range(8):
                lo, hi = max(j, b * R), min(j + 128, b * R + R)
                if lo < hi:
                    B = (NT - 1 - i) * 8 + b
                    unit = G.at[NA + lax.rem(B, NS), B // (2 * NS), lax.rem(B // NS, 2)]
                    unit[lo - b * R : hi - b * R] = rows[lo - j : hi - j]

    def down_grads(r, layer, sd):
        def product(i):
            for j in range(0, W, 256):
                n = min(256, W - j)
                sd[:, j : j + n] = dot(dyT[...], hids[lax.rem(i, 2), :, j : j + n]).astype(BF16)
            start(hid_in(layer, jnp.minimum(i + 2, NT - 1), i))

        product(0)
        stream_a(1, r)

        @pl.loop(1, NT)
        def _(i):
            wait(hid_in(layer, i, i))
            turn_units(sd, i - 1)
            product(i)

        turn_units(sd, NT - 1)
        stream_b(0, layer)
        stream_a(3, r - 1)
        wait(hid_in(layer, 0, 0), hid_in(layer, 0, 1))

    def da_at(ci):
        return (gu2, gu3)[ci // 2].at[ci % 2]

    def output_grad(ci):
        step = CH // 2

        @pl.loop(0, 2)
        def _(j):
            r = span(ci * 2 + j, step)
            h = dgu[r, :W].astype(F32)
            s = scale_of(h)
            d = da_at(ci)[span(j, step), :].astype(BF16).astype(F32)
            n = dy[r, :] + (s * (d - h * (s * s * jnp.mean(d * h, -1, keepdims=True)))).astype(BF16)
            dy[r, :] = n
            dyT[:, r] = n.T

    swap = [copy(s, d, tsem.at[i]) for i, (s, d) in enumerate(((h1_ref, dgu.at[:, pl.ds(0, W)]), (a0_ref, a), (a0T_ref, aT)))]

    def turn():
        wait(*swap)
        output_grad(0)
        output_grad(1)
        output_grad(2)
        output_grad(3)
        stream_a(2, NT - 1)
        stream_b(1, 1)

    first = [copy(a1_ref, a, tsem.at[0]), copy(dy_ref.at[0], dy, tsem.at[1]), copy(a1T_ref, aT, tsem.at[2]), copy(dyT_ref, dyT, tsem.at[3])]
    start(first[0], *tiles(0), down(0), *first[1:])
    ssacc[...] = jnp.zeros_like(ssacc)
    for ci in range(NC):
        da_at(ci)[...] = jnp.zeros((CH, D), F32)
    wait(*first[:2])

    @pl.loop(0, 2 * NT)
    def _(r):
        slot = lax.rem(r, 2)

        wait(*tiles(r), down(r))

        @pl.when(r + 1 < 2 * NT)
        def _():
            start(*tiles(r + 1), down(r + 1))

        @pl.when((r >= 1) & (r < NT))
        def _():
            wait(hid_out(r - 1))

        def A(ci):
            rows = pl.ds(ci * CH, CH)
            gu = dot(a[rows, :], wgu[slot])
            gus[ci % 2][0] = gu[:, :W]
            gus[ci % 2][1] = gu[:, W:]
            dhs[ci % 2][...] = dot_nt(dy[rows, :], wd[slot]).astype(BF16)

        def E(ci):
            rows = pl.ds(ci * CH, CH)
            gu = gus[ci % 2]
            g, u, d = gu[0], gu[1], dhs[ci % 2][...].astype(F32)
            s = sigmoid(g)
            silu = g * s
            hids[0, rows, :] = (silu * u).astype(BF16)
            dgu[rows, :W] = (d * u * (s + silu * (1.0 - s))).astype(BF16)
            dgu[rows, W:] = (d * silu).astype(BF16)

        for ci in range(NC):
            A(ci)
            if ci:
                E(ci - 1)
        E(NC - 1)

        @pl.when(r < NT - 1)
        def _():
            start(hid_out(r))

        @pl.when(r == 0)
        def _():
            pl.semaphore_wait(bar, peers - 1)
            wait(*first[2:])

        usual = (r != NT) & (r != NT + 2)

        @pl.when((r >= 1) & usual)
        def _():
            stream_a(1, r - 1)

            @pl.when(r >= 2)
            def _():
                stream_a(3, r - 2)

            @pl.when(r == NT + 1)
            def _():
                start(hid_in(0, 0, 0), hid_in(0, 1, 1))
                stream_b(3, 1)

        @pl.when(r == NT + 2)
        def _():
            stream_b(1, 0)

        gate_up_grads(r)
        stream_a(0, r)

        @pl.when(r < NT)
        def _():
            for ci in range(NC):
                da_at(ci)[...] += dot_nt(dgu[pl.ds(ci * CH, CH), :], wgu[slot])

        @pl.when((r >= 1) & usual)
        def _():
            stream_a(2, r - 1)

        @pl.when((r >= NT - 1) & (r < NT + 4))
        def _():
            @pl.when(r == NT)
            def _():
                stream_b(2, 1)

            @pl.when(r == NT + 3)
            def _():
                stream_b(2, 0)

            @pl.when((r == NT - 1) | (r == NT + 1))
            def _():
                layer = (NT + 1 - r) // 2

                @pl.when(layer == 1)
                def _():
                    start(*swap, hid_in(1, 1, 1))

                @pl.when(layer == 0)
                def _():
                    wait(hid_in(0, 0, 0))

                down_grads(r, layer, wd.at[slot])

                @pl.when(layer == 1)
                def _():
                    turn()

                @pl.when(layer == 0)
                def _():
                    stream_a(2, r)

    R2 = NS * R

    def block(ref, i, layer, t):
        return ref.at[layer, span(i, R), span(t, W)]

    def nw(e, layer, t):
        return hids.at[e, span(layer * NT + t, R)]

    @pl.loop(0, NT)
    def _(t):
        for layer in range(2):
            for i, ref in enumerate((mg_ref, vg_ref, mu_ref, vu_ref)):
                start(copy(block(ref, 0, layer, t), gus[i].at[layer, span(t, R)], msem.at[i]))
            for e, ref in enumerate((wg_ref, wu_ref)):
                start(copy(block(ref, me, layer, t), nw(e, layer, t), nsem.at[e]))

    def arrived(ref, sem):
        wait(copy(ref, ref, sem))

    own_down = [copy(wd_ref.at[layer, span(me, R2), :], a.at[pl.ds(layer * R2, R2)], nsem.at[2 + layer]) for layer in range(2)]
    start(*own_down)

    last = 2 * NT - 1
    stream_a(1, last)
    stream_a(3, last - 1)
    stream_a(2, last)
    stream_b(3, 0)
    stream_a(3, last)

    lanes = ssall.shape[-1]
    part = ssacc[:, :lanes]
    for j in range(1, W // lanes):
        part = part + ssacc[:, j * lanes : (j + 1) * lanes]
    ssall[me] = part
    parts = [remote(ssall.at[me], ssall.at[me], sS.at[j], rS.at[j], lax.rem(me + j, peers)) for j in range(1, peers)]
    start(*parts)
    wait(*parts)
    total = ssall[0]
    for j in range(1, peers):
        total = total + ssall[j]
    total = jnp.sum(jnp.sum(total, 0, keepdims=True), 1, keepdims=True)
    fac = jnp.minimum(1.0, 0.5 * lax.rsqrt(total / z.count + 1e-30))
    fac_ref[...] = jnp.broadcast_to(fac, fac_ref.shape)

    def new_weight(w, m, v, g):
        w, g = w.astype(F32), g.astype(F32) * fac
        m = 0.9 * m + 0.1 * g
        v = 0.95 * v + 0.05 * g * g
        return (w - 0.02 * (m * lax.rsqrt(v + 1e-8) + 0.1 * w)).astype(BF16)

    outs = (og_ref, ou_ref)
    chunks = [(e, layer) for e in range(2) for layer in range(2)]

    def here(q, j):
        e, layer = chunks[q]
        return outs[e].at[layer, span(chip(j) * 2 + k, R)]

    def send(q, j, send, recv, to):
        return remote(here(q, j), here(q, j), send, recv, to)

    def right_of(q):
        return send(q, 0, sR.at[q], rR.at[q], chip(1) * 2 + k)

    def left_of(q):
        return send(q, 0, sL.at[q], rL.at[q], chip(-1) * 2 + k)

    def across(q):
        j = chunks[q][0] * 2 - 1
        return send(q, j, sX.at[q], rX.at[q], chip(-j) * 2 + k)

    def over(q, i):
        return send(q, (0, -1, 1, 2)[i], sD.at[q, i], rD.at[q, i], partner)

    def leave(q):
        arrived(here(q, 0), lsem.at[q])
        start(right_of(q), left_of(q), over(q, 0))

    for q, (e, layer) in enumerate(chunks):
        if layer == 0:
            arrived(hids.at[e, pl.ds(0, 2 * NT * R)], nsem.at[e])
            for i in (2 * e, 2 * e + 1):
                arrived(gus[i].at[:, pl.ds(0, NT * R)], msem.at[i])

        @pl.loop(0, NT)
        def _(t):
            held = span(t, R)
            own = nw(e, layer, t)
            own[...] = new_weight(own[...], gus[2 * e][layer, held], gus[2 * e + 1][layer, held], (gg_ref, gup_ref)[e][layer, :, span(t, W)])
            start(copy(own, block(outs[e], me, layer, t), lsem.at[q]))

        if q:
            leave(q - 1)
    leave(len(chunks) - 1)
    moments = [copy(ref, gus[i].at[:, pl.ds(0, R2)], msem.at[i]) for i, ref in enumerate((md_ref, vd_ref))]
    start(*moments)
    wait(*own_down, *moments)

    @pl.loop(0, NS)
    def _(i):
        for layer in range(2):
            held, own = span(i, R), span(layer * NS + i, R)
            a[own, :] = new_weight(a[own, :], gus[0][layer, held], gus[1][layer, held], gd_ref[layer, held])

    places = (n0_ref.at[0], n1_ref.at[0], nd_ref.at[0], nd_ref.at[1])
    new_down = [copy(a.at[pl.ds(i % 2 * R2, R2)], place, nsem.at[i]) for i, place in enumerate(places)]
    start(*new_down)
    for q, (e, layer) in enumerate(chunks):
        right_of(q).wait_recv()
        if e == 0:
            start(across(q))
        start(over(q, 1))
        left_of(q).wait_recv()
        if e:
            start(across(q))
        start(over(q, 2))
    for q in range(len(chunks)):
        across(q).wait_recv()
        start(over(q, 3))
    wait(*new_down)
    for q in range(len(chunks)):
        wait(*[over(q, i) for i in range(4)])
        for sent in (right_of(q), left_of(q), across(q)):
            sent.wait_send()


def copy_kernel(og_ref, ou_ref, ng_ref, nu_ref, buf, isem, osem):
    n, rows = buf.shape[:2]
    per = n // 2
    ins, outs = [], []
    for i in range(n):
        src, dst = ((og_ref, ng_ref), (ou_ref, nu_ref))[i // per]
        at = pl.ds(i % per * rows, rows)
        ins.append(copy(src.at[at], buf.at[i], isem.at[i]))
        outs.append(copy(buf.at[i], dst.at[at], osem.at[i]))
    start(*ins)
    for i in range(n):
        wait(ins[i])
        start(outs[i])
    wait(*outs)


def moments_kernel(fac_ref, *refs):
    ins, outs = refs[:9], refs[9:]
    for i in range(3):
        m, v, g = (r[0] for r in ins[3 * i : 3 * i + 3])
        g = g.astype(F32) * fac_ref[:1, :1]
        outs[2 * i][0] = 0.9 * m + 0.1 * g
        outs[2 * i + 1][0] = 0.95 * v + 0.05 * g * g


def place_kernel(firsts, at_ref, *refs):
    out, sem = refs[-2:]
    copies = []
    for i, first in enumerate(firsts):
        count, rows = refs[i].shape[:2]
        copies.append(copy(refs[i], out.at[pl.ds(first, count), pl.ds(pl.multiple_of(at_ref[i] * rows, 16), rows)], sem.at[i]))
    start(*copies)
    wait(*copies)


VMEM, HBM = pl.BlockSpec(memory_space=pltpu.VMEM), pl.BlockSpec(memory_space=pl.ANY)
dma = pltpu.SemaphoreType.DMA


def bf16(*shape):
    return pltpu.VMEM(shape, BF16)


def f32(*shape):
    return pltpu.VMEM(shape, F32)


def call(kernel, ins, out, scratch, cost, limit=VMEM_LIMIT, **params):
    flops, moved = cost
    more = {key: params.pop(key) for key in ("grid", "input_output_aliases") if key in params}
    outs = [spec for _, _, spec in out]
    shapes = [jax.ShapeDtypeStruct(shape, dtype) for shape, dtype, _ in out]
    return pl.pallas_call(
        kernel,
        out_shape=shapes,
        in_specs=ins,
        out_specs=outs,
        scratch_shapes=scratch,
        compiler_params=pltpu.CompilerParams(vmem_limit_bytes=limit, **params),
        cost_estimate=pl.CostEstimate(flops=int(flops), bytes_accessed=int(moved), transcendentals=0),
        **more,
    )


def solution(mesh):
    n = mesh.shape["dp"]
    chips = n // 2

    def ring(shift, flip=0):
        return [(i, (i // 2 + shift) % chips * 2 + (i + flip) % 2) for i in range(n)]

    def right(t):
        return lax.ppermute(t, "dp", ring(1))

    def left(t):
        return lax.ppermute(t, "dp", ring(-1))

    def partner(t):
        return lax.ppermute(t, "dp", ring(0, 1))

    def step(x, dy, *arrays):
        weights, m, v = (arrays[i : i + 3] for i in (0, 3, 6))
        wg, wu, wd = weights
        T, D = x.shape[1:]
        layers, _, FF = wg.shape
        W, CH = D, 512
        NT, NC, R = FF // W, T // CH, D // n
        NS = FF // n // R
        z = SimpleNamespace(T=T, D=D, FF=FF, W=W, CH=CH, NT=NT, NC=NC, R=R, NS=NS, chips=chips, count=float(sum(w.size for w in weights)))
        tokens, turned, hidden = ((T, D), BF16, HBM), ((D, T), BF16, HBM), ((layers, NT, T, W), BF16, HBM)
        h1, a1, a1T, a0, a0T, dyT, hid = call(
            functools.partial(forward_kernel, z), [VMEM] + [HBM] * 4,
            [tokens, tokens, turned, tokens, turned, turned, hidden],
            [*[bf16(T, D)] * 2, *[bf16(D, T)] * 2, *[bf16(T, D)] * 2, bf16(D, T), bf16(2, D, 2 * W), bf16(FF, D), bf16(T, FF), *[f32(2, CH, W)] * 2,
             dma((2, 2)), dma((2,)), dma((NT,)), dma((NC + 1, 3))],
            (6 * T * D * FF, 8 * T * FF),
        )(x, dy, wg, wu, wd)
        slots = 6 + NS
        blocks = bf16(slots, R, W)
        flat, tall, half, gathered = (layers, R, FF), (layers, NS * R, D), (1, NS * R, D), (layers, D, FF)
        gg, gup, gd, fac, nd, n0, n1, og, ou, _ = call(
            functools.partial(backward_kernel, z), [HBM] * 17,
            [(flat, BF16, VMEM), (flat, BF16, VMEM), (tall, BF16, VMEM), ((8, 128), F32, VMEM), (tall, BF16, HBM), (half, BF16, HBM), (half, BF16, HBM),
             (gathered, BF16, HBM), (gathered, BF16, HBM), hidden],
            [bf16(T, D), bf16(D, T), bf16(T, D), bf16(D, T), bf16(2, D, 2 * W), bf16(2, W, D), *[f32(2, CH, W)] * 4, *[bf16(CH, W)] * 2,
             bf16(2, T, W), bf16(T, 2 * W),
             bf16(slots, chips, 2, R, W), bf16(slots, chips, R, W), blocks, blocks, blocks, f32(8, W), f32(n, 8, 128),
             dma((2, 2)), dma((2,)), dma((4,)), dma((2,)), *[dma((slots,))] * 8, dma((n,)), dma((n,)),
             *[dma((4,))] * 9, *[dma((4, 4))] * 2],
            (24 * T * D * FF, 8 * T * FF), collective_id=0, has_side_effects=True, input_output_aliases={16: 9},
        )(h1, a1, a1T, a0, a0T, dyT, dy, wg, wu, wd, m[0], v[0], m[1], v[1], m[2], v[2], hid)

        me = lax.axis_index("dp")
        c, k = me // 2, lax.rem(me, 2)

        def place(out, pieces):
            ts = [t for t, _, _ in pieces]
            count = len(ts)
            known = () if out is None else (out,)
            return call(
                functools.partial(place_kernel, [first for _, _, first in pieces]),
                [pl.BlockSpec(memory_space=pltpu.SMEM)] + [VMEM] * count + [HBM] * len(known), [(wd.shape, BF16, HBM)], [dma((count,))],
                (2e6 * count, 4 * sum(t.size for t in ts)), 1 << 24, input_output_aliases={count + 1: 0} if known else {},
            )(jnp.stack([at for _, at, _ in pieces]).astype(jnp.int32), *ts, *known)[0]

        def spot(shift, core):
            return lax.rem(c + shift + chips, chips) * 2 + core

        left0, right1 = right(n0), left(n1)
        left1, right0 = right(n1), left(n0)
        p_own = partner(nd)
        rows = layers * D
        parts = [(rows, FF), BF16, HBM]
        ng, nu = call(
            copy_kernel, [HBM] * 2, [parts] * 2, [bf16(8, rows // 4, FF), dma((8,)), dma((8,))], (12e9, 8 * rows * FF),
        )(og.reshape(rows, FF), ou.reshape(rows, FF))
        opp = right(left0), left(right1)
        kinds = [(shape, pl.BlockSpec((1, *shape[1:]), lambda i: (i, 0, 0))) for shape in (flat, flat, tall)]
        moved = call(
            moments_kernel, [pl.BlockSpec((8, 128), lambda i: (0, 0))] + [spec for _, spec in kinds for _ in range(3)],
            [(shape, F32, spec) for shape, spec in kinds for _ in range(2)], [], (10e9, 54 * m[0].size), grid=(layers,),
        )(fac, *[t for i, g in enumerate((gg, gup, gd)) for t in (m[i], v[i], g)])
        p_sides = [partner(t) for t in (left0, right1, left1, right0)]
        pieces = [(nd, spot(0, k), 0), (p_own, spot(0, 1 - k), 0)]
        for t, p, (j, first) in zip((left0, right1, left1, right0), p_sides, ((-1, 0), (1, 1), (-1, 1), (1, 0)), strict=True):
            pieces += [(t, spot(j, k), first), (p, spot(j, 1 - k), first)]
        out = place(None, pieces)
        p_opp = [partner(t) for t in opp]
        out = place(out, [piece for i in range(2) for piece in ((opp[i], spot(2, k), i), (p_opp[i], spot(2, 1 - k), i))])
        return ng.reshape(gathered), nu.reshape(gathered), out, *moved[::2], *moved[1::2]

    whole, split = P(None, None, None), P(None, "dp", None)
    step = jax.shard_map(
        step,
        mesh=mesh,
        in_specs=(P(("rep", "dp")),) * 2 + (whole,) * 3 + (split,) * 6,
        out_specs=(P("rep", None, None),) * 3 + (P("rep", "dp", None),) * 6,
        check_vma=False,
    )
    return step
```

```python
import functools
from types import SimpleNamespace

import jax
import jax.numpy as jnp
from jax import lax
from jax.experimental import pallas as pl
from jax.experimental.pallas import tpu as pltpu
from jax.sharding import PartitionSpec as P

F32, BF16 = jnp.float32, jnp.bfloat16
VMEM_LIMIT = 67043328
NT_DIMS = (((1,), (1,)), ((), ()))
copy = pltpu.make_async_copy


def dot(a, b):
    return jnp.dot(a, b, preferred_element_type=F32)


def dot_nt(a, b):
    return lax.dot_general(a, b, NT_DIMS, preferred_element_type=F32)


def sigmoid(g):
    return 0.5 * jnp.tanh(0.5 * g) + 0.5


def scale_of(h):
    return lax.rsqrt(jnp.mean(h * h, -1, keepdims=True) + 1e-6)


def span(i, n):
    return pl.ds(pl.multiple_of(i * n, n), n)


def start(*copies):
    for c in copies:
        c.start()


def wait(*copies):
    for c in copies:
        c.wait()


def gate_up_tiles(z, layer_of, wg_ref, wu_ref, wgu, sem):
    def copies(t):
        slot = lax.rem(t, 2)
        return [
            copy(ref.at[layer_of(t), :, span(lax.rem(t, z.NT), z.W)], wgu.at[slot, :, pl.ds(e * z.W, z.W)], sem.at[slot, e])
            for e, ref in enumerate((wg_ref, wu_ref))
        ]

    return copies


def forward_kernel(z, x_ref, dy_ref, wg_ref, wu_ref, wd_ref, h1_ref, a1_ref, a1T_ref, a0_ref, a0T_ref, dyT_ref, hid_ref,
                   x, a, a1, aT, cT, h1, dy, dyT, wgu, wd, hid, gu0, gu1, wsem, dsem, hsem, tsem):
    W, CH, NT, NC, T = z.W, z.CH, z.NT, z.NC, z.T
    gus = (gu0, gu1)
    tiles = gate_up_tiles(z, lambda t: 0, wg_ref, wu_ref, wgu, wsem)
    states, later, down = copy(x_ref.at[0], x, dsem.at[0]), copy(dy_ref.at[0], dy, dsem.at[1]), copy(wd_ref.at[0], wd, dsem.at[2])
    start(states, *tiles(0), later)
    wait(states)
    step = CH // 2
    for i in range(T // step):
        r = pl.ds(i * step, step)
        h = x[r, :].astype(F32)
        a[r, :] = (h * scale_of(h)).astype(BF16)
    pairs = (a, a0_ref), (aT, a0T_ref), (dyT, dyT_ref)
    whole = [copy(s, d, tsem.at[0, e]) for e, (s, d) in enumerate(pairs)]
    wait(later)

    def hid_out(t):
        return copy(hid.at[:, span(t, W)], hid_ref.at[0, t], hsem.at[t])

    @pl.loop(0, NT)
    def _(t):
        wait(*tiles(t))

        @pl.when(t + 1 < NT)
        def _():
            start(*tiles(t + 1))

        @pl.when(t == 1)
        def _():
            start(down)

        turned = span(jnp.minimum(t, NC - 1), CH)
        aT[:, turned] = a[turned, :].T
        dyT[:, turned] = dy[turned, :].T

        def E(c):
            g, u = gus[c % 2][0], gus[c % 2][1]
            hid[pl.ds(c * CH, CH), span(t, W)] = (g * sigmoid(g) * u).astype(BF16)

        for c in range(NC):
            gu = dot(a[pl.ds(c * CH, CH), :], wgu[lax.rem(t, 2)])
            gus[c % 2][0] = gu[:, :W]
            gus[c % 2][1] = gu[:, W:]
            if c:
                E(c - 1)
        E(NC - 1)
        start(hid_out(t))

    start(*whole)
    wait(down)

    def project(i):
        r = span(i, CH)
        h1[r, :] = x[r, :] + dot(hid[r, :], wd[...]).astype(BF16)

    def norm(i):
        r = span(i, CH)
        h = h1[r, :].astype(F32)
        n = (h * scale_of(h)).astype(BF16)
        a1[r, :] = n
        cT[:, r] = n.T

    def done(i):
        r = span(i, CH)
        parts = (h1.at[r], h1_ref.at[r]), (a1.at[r], a1_ref.at[r]), (cT.at[:, r], a1T_ref.at[:, r])
        return [copy(s, d, tsem.at[1 + i, e]) for e, (s, d) in enumerate(parts)]

    project(0)

    @pl.loop(1, NC)
    def _(i):
        norm(i - 1)
        project(i)
        start(*done(i - 1))

    norm(NC - 1)
    start(*done(NC - 1))
    wait(*whole, *[d for i in range(NC) for d in done(i)], *[hid_out(t) for t in range(NT)])


def backward_kernel(z, h1_ref, a1_ref, a1T_ref, a0_ref, a0T_ref, dyT_ref, dy_ref, wg_ref, wu_ref, wd_ref,
                    mg_ref, vg_ref, mu_ref, vu_ref, md_ref, vd_ref, _,
                    gg_out, gup_out, gd_out, fac_out, nd_ref, n0_ref, n1_ref, og_ref, ou_ref, hid_ref,
                    a, aT, dy, dyT, wgu, wd, gu0, gu1, gu2, gu3, dh0, dh1, hids, dgu,
                    G, PB, OB, B1, B2, gg_ref, gup_ref, gd_ref, fac_ref, ssacc, ssall,
                    wsem, dsem, tsem, hsem, sP, rP, sO, rO, s1, r1, s2, r2, sS, rS,
                    msem, nsem, lsem, sR, rR, sL, rL, sX, rX, sD, rD):
    W, CH, NT, NC, D, R, NS = z.W, z.CH, z.NT, z.NC, z.D, z.R, z.NS
    NA = 6
    peers = 2 * z.chips
    gus, dhs = (gu0, gu1, gu2, gu3), (dh0, dh1)
    rep, me = lax.axis_index("rep"), lax.axis_index("dp")
    c, k = me // 2, lax.rem(me, 2)

    def chip(j):
        return lax.rem(c + j + z.chips, z.chips)

    def remote(src, dst, send, recv, to):
        return pltpu.make_async_remote_copy(src_ref=src, dst_ref=dst, send_sem=send, recv_sem=recv, device_id=(rep, to),
                                            device_id_type=pl.DeviceIdType.MESH)

    bar = pltpu.get_barrier_semaphore()
    for j in range(1, peers):
        pl.semaphore_signal(bar, inc=1, device_id=(rep, lax.rem(me + j, peers)), device_id_type=pl.DeviceIdType.MESH)

    partner = c * 2 + 1 - k

    def copyP(s):
        return remote(G.at[s, :, 1 - k], PB.at[s], sP.at[s], rP.at[s], partner)

    def copyO(s, d):
        return remote(G.at[s, chip(2), k], OB.at[s], sO.at[s], rO.at[s], chip(d) * 2 + k)

    def copy1(s, d):
        return remote(G.at[s, chip(-d), k], B1.at[s], s1.at[s], r1.at[s], chip(-d) * 2 + k)

    def copy2(s, d):
        return remote(G.at[s, chip(d), k], B2.at[s], s2.at[s], r2.at[s], chip(d) * 2 + k)

    def both(s, q):
        return G[s, q, k].astype(F32) + PB[s, q].astype(F32)

    def stage0(each):
        each(lambda s, d, put: copyP(s).start())

    def stage1(each):
        def add(s, d, put):
            for q in (chip(2), chip(-d)):
                G[s, q, k] = both(s, q).astype(BF16)

        each(lambda s, d, put: copyP(s).wait_recv())
        each(add)
        each(lambda s, d, put: copyO(s, d).start())
        each(lambda s, d, put: copy1(s, d).start())

    def stage2(each):
        def add(s, d, put):
            q = chip(d)
            G[s, q, k] = (both(s, q) + OB[s].astype(F32)).astype(BF16)

        each(lambda s, d, put: copyO(s, d).wait_recv())
        each(add)
        each(lambda s, d, put: copy2(s, d).start())

    def stage3(each):
        def arrive(s, d, put):
            copy1(s, d).wait_recv()
            copy2(s, d).wait_recv()

        def add(s, d, put):
            g = (both(s, c) + (B1[s].astype(F32) + B2[s].astype(F32))).astype(BF16)
            put(g)
            w = g.astype(F32)
            ssacc[...] += jnp.sum((w * w).reshape(-1, *ssacc.shape), 0)

        def sent(s, d, put):
            for cp in (copyP(s), copyO(s, d), copy1(s, d), copy2(s, d)):
                cp.wait_send()

        for f in (arrive, add, sent):
            each(f)

    stages = stage0, stage1, stage2, stage3

    def a_slot(r, e):
        return lax.rem(r * 2 + e, NA)

    def a_put(r, e):
        def put(g):
            (gg_ref, gup_ref)[e][1 - r // NT, :, span(lax.rem(r, NT), W)] = g

        return put

    def stream_a(stage, r):
        stages[stage](lambda f: [f(a_slot(r, e), d, a_put(r, e)) for e, d in enumerate((1, -1))])

    def stream_b(stage, layer):
        def put(i):
            def f(g):
                gd_ref[layer, span(i, R), :] = g

            return f

        stages[stage](lambda f: pl.loop(0, NS)(lambda i: f(NA + i, lax.rem(i + layer, 2) * 2 - 1, put(i))))

    def layer_of(r):
        return 1 - r // NT

    tiles = gate_up_tiles(z, layer_of, wg_ref, wu_ref, wgu, wsem)

    def down(r):
        slot = lax.rem(r, 2)
        return copy(wd_ref.at[layer_of(r), span(lax.rem(r, NT), W), :], wd.at[slot], dsem.at[slot])

    def hid_out(t):
        return copy(hids.at[0], hid_ref.at[1, t], hsem.at[0])

    def gate_up_grads(r):
        for j in range(0, 2 * W, 256):
            gw = dot(aT[...], dgu[:, j : j + 256]).astype(BF16)
            for i in range(0, 256, 128):
                e, q = divmod(j + i, W)
                G[a_slot(r, e), :, :, :, q : q + 128] = gw[:, i : i + 128].reshape(*G.shape[1:4], 128)

    def hid_in(layer, i, slot):
        return copy(hid_ref.at[layer, NT - 1 - i], hids.at[lax.rem(slot, 2)], hsem.at[lax.rem(slot, 2)])

    def turn_units(sd, i):
        for j in range(0, W, 128):
            rows = sd[:, j : j + 128].T
            for b in range(8):
                lo, hi = max(j, b * R), min(j + 128, b * R + R)
                if lo < hi:
                    B = (NT - 1 - i) * 8 + b
                    unit = G.at[NA + lax.rem(B, NS), B // (2 * NS), lax.rem(B // NS, 2)]
                    unit[lo - b * R : hi - b * R] = rows[lo - j : hi - j]

    def down_grads(r, layer, sd):
        def product(i):
            for j in range(0, W, 256):
                n = min(256, W - j)
                sd[:, j : j + n] = dot(dyT[...], hids[lax.rem(i, 2), :, j : j + n]).astype(BF16)
            start(hid_in(layer, jnp.minimum(i + 2, NT - 1), i))

        product(0)
        stream_a(1, r)

        @pl.loop(1, NT)
        def _(i):
            wait(hid_in(layer, i, i))
            turn_units(sd, i - 1)
            product(i)

        turn_units(sd, NT - 1)
        stream_b(0, layer)
        stream_a(3, r - 1)
        wait(hid_in(layer, 0, 0), hid_in(layer, 0, 1))

    def da_at(ci):
        return (gu2, gu3)[ci // 2].at[ci % 2]

    def output_grad(ci):
        step = CH // 2

        @pl.loop(0, 2)
        def _(j):
            r = span(ci * 2 + j, step)
            h = dgu[r, :W].astype(F32)
            s = scale_of(h)
            d = da_at(ci)[span(j, step), :].astype(BF16).astype(F32)
            n = dy[r, :] + (s * (d - h * (s * s * jnp.mean(d * h, -1, keepdims=True)))).astype(BF16)
            dy[r, :] = n
            dyT[:, r] = n.T

    swap = [copy(s, d, tsem.at[i]) for i, (s, d) in enumerate(((h1_ref, dgu.at[:, pl.ds(0, W)]), (a0_ref, a), (a0T_ref, aT)))]

    def turn():
        wait(*swap)
        output_grad(0)
        output_grad(1)
        output_grad(2)
        output_grad(3)
        stream_a(2, NT - 1)
        stream_b(1, 1)

    first = [copy(a1_ref, a, tsem.at[0]), copy(dy_ref.at[0], dy, tsem.at[1]), copy(a1T_ref, aT, tsem.at[2]), copy(dyT_ref, dyT, tsem.at[3])]
    start(first[0], *tiles(0), down(0), first[1])
    ssacc[...] = jnp.zeros_like(ssacc)
    for ci in range(NC):
        da_at(ci)[...] = jnp.zeros((CH, D), F32)
    wait(*first[:2])
    start(*first[2:])

    @pl.loop(0, 2 * NT)
    def _(r):
        slot = lax.rem(r, 2)

        wait(*tiles(r), down(r))

        @pl.when(r + 1 < 2 * NT)
        def _():
            start(*tiles(r + 1), down(r + 1))

        @pl.when((r >= 1) & (r < NT))
        def _():
            wait(hid_out(r - 1))

        def A(ci):
            rows = pl.ds(ci * CH, CH)
            gu = dot(a[rows, :], wgu[slot])
            gus[ci % 2][0] = gu[:, :W]
            gus[ci % 2][1] = gu[:, W:]
            dhs[ci % 2][...] = dot_nt(dy[rows, :], wd[slot]).astype(BF16)

        def E(ci):
            rows = pl.ds(ci * CH, CH)
            gu = gus[ci % 2]
            g, u, d = gu[0], gu[1], dhs[ci % 2][...].astype(F32)
            s = sigmoid(g)
            silu = g * s
            hids[r // NT, rows, :] = (silu * u).astype(BF16)
            dgu[rows, :W] = (d * u * (s + silu * (1.0 - s))).astype(BF16)
            dgu[rows, W:] = (d * silu).astype(BF16)

        for ci in range(NC):
            A(ci)
            if ci:
                E(ci - 1)

        @pl.when(r == 0)
        def _():
            pl.semaphore_wait(bar, peers - 1)
            wait(*first[2:])

        usual = (r != NT) & (r != NT + 2)

        @pl.when((r >= 1) & usual)
        def _():
            stream_a(1, r - 1)

            @pl.when(r >= 2)
            def _():
                stream_a(3, r - 2)

            @pl.when(r == NT + 1)
            def _():
                start(hid_in(0, 0, 0))
                stream_b(3, 1)

        @pl.when(r == NT + 2)
        def _():
            stream_b(1, 0)

        E(NC - 1)
        gate_up_grads(r)
        stream_a(0, r)

        @pl.when(r < NT - 1)
        def _():
            start(hid_out(r))

        @pl.when(r < NT)
        def _():
            for ci in range(NC):
                da_at(ci)[...] += dot_nt(dgu[pl.ds(ci * CH, CH), :], wgu[slot])

        @pl.when((r >= 1) & usual)
        def _():
            stream_a(2, r - 1)

        @pl.when((r >= NT - 1) & (r < NT + 4))
        def _():
            @pl.when(r == NT)
            def _():
                stream_b(2, 1)

            @pl.when(r == NT + 3)
            def _():
                stream_b(2, 0)

            @pl.when((r == NT - 1) | (r == NT + 1))
            def _():
                layer = (NT + 1 - r) // 2

                @pl.when(layer == 1)
                def _():
                    start(*swap, hid_in(1, 1, 1))

                @pl.when(layer == 0)
                def _():
                    start(hid_in(0, 1, 1))
                    wait(hid_in(0, 0, 0))

                down_grads(r, layer, wd.at[slot])

                @pl.when(layer == 1)
                def _():
                    turn()

                @pl.when(layer == 0)
                def _():
                    stream_a(2, r)

    R2 = NS * R

    def block(ref, i, layer, t):
        return ref.at[layer, span(i, R), span(t, W)]

    def nw(e, layer, t):
        return hids.at[e, span(layer * NT + t, R)]

    @pl.loop(0, NT)
    def _(t):
        for layer in range(2):
            for i, ref in enumerate((mg_ref, vg_ref, mu_ref, vu_ref)):
                start(copy(block(ref, 0, layer, t), gus[i].at[layer, span(t, R)], msem.at[i]))
            for e, ref in enumerate((wg_ref, wu_ref)):
                start(copy(block(ref, me, layer, t), nw(e, layer, t), nsem.at[e]))

    def arrived(ref, sem):
        wait(copy(ref, ref, sem))

    own_down = [copy(wd_ref.at[layer, span(me, R2), :], a.at[pl.ds(layer * R2, R2)], nsem.at[2 + layer]) for layer in range(2)]
    start(*own_down)

    last = 2 * NT - 1
    stream_a(1, last)
    stream_a(3, last - 1)
    stream_a(2, last)
    stream_b(3, 0)
    stream_a(3, last)

    lanes = ssall.shape[-1]
    part = ssacc[:, :lanes]
    for j in range(1, W // lanes):
        part = part + ssacc[:, j * lanes : (j + 1) * lanes]
    ssall[me] = part
    parts = [remote(ssall.at[me], ssall.at[me], sS.at[j], rS.at[j], lax.rem(me + j, peers)) for j in range(1, peers)]
    start(*parts)
    wait(*parts)
    total = ssall[0]
    for j in range(1, peers):
        total = total + ssall[j]
    total = jnp.sum(jnp.sum(total, 0, keepdims=True), 1, keepdims=True)
    fac = jnp.minimum(1.0, 0.5 * lax.rsqrt(total / z.count + 1e-30))
    fac_ref[...] = jnp.broadcast_to(fac, fac_ref.shape)
    pairs = (gg_ref, gg_out), (gup_ref, gup_out), (gd_ref, gd_out), (fac_ref, fac_out)
    leaving = [copy(s, d, tsem.at[i]) for i, (s, d) in enumerate(pairs)]
    start(*leaving)

    def new_weight(w, m, v, g):
        w, g = w.astype(F32), g.astype(F32) * fac
        m = 0.9 * m + 0.1 * g
        v = 0.95 * v + 0.05 * g * g
        return (w - 0.02 * (m * lax.rsqrt(v + 1e-8) + 0.1 * w)).astype(BF16)

    outs = (og_ref, ou_ref)
    chunks = [(e, layer) for e in range(2) for layer in range(2)]

    def here(q, j):
        e, layer = chunks[q]
        return outs[e].at[layer, span(chip(j) * 2 + k, R)]

    def send(q, j, send, recv, to):
        return remote(here(q, j), here(q, j), send, recv, to)

    def right_of(q):
        return send(q, 0, sR.at[q], rR.at[q], chip(1) * 2 + k)

    def left_of(q):
        return send(q, 0, sL.at[q], rL.at[q], chip(-1) * 2 + k)

    def across(q):
        j = chunks[q][0] * 2 - 1
        return send(q, j, sX.at[q], rX.at[q], chip(-j) * 2 + k)

    def over(q, i):
        return send(q, (0, -1, 1, 2)[i], sD.at[q, i], rD.at[q, i], partner)

    def leave(q):
        arrived(here(q, 0), lsem.at[q])
        start(right_of(q), left_of(q), over(q, 0))

    for q, (e, layer) in enumerate(chunks):
        if layer == 0:
            arrived(hids.at[e, pl.ds(0, 2 * NT * R)], nsem.at[e])
            for i in (2 * e, 2 * e + 1):
                arrived(gus[i].at[:, pl.ds(0, NT * R)], msem.at[i])

        @pl.loop(0, NT)
        def _(t):
            held = span(t, R)
            own = nw(e, layer, t)
            own[...] = new_weight(own[...], gus[2 * e][layer, held], gus[2 * e + 1][layer, held], (gg_ref, gup_ref)[e][layer, :, span(t, W)])
            start(copy(own, block(outs[e], me, layer, t), lsem.at[q]))

        if q:
            leave(q - 1)
    leave(len(chunks) - 1)
    moments = [copy(ref, gus[i].at[:, pl.ds(0, R2)], msem.at[i]) for i, ref in enumerate((md_ref, vd_ref))]
    start(*moments)
    wait(*own_down, *moments)

    @pl.loop(0, NS)
    def _(i):
        for layer in range(2):
            held, own = span(i, R), span(layer * NS + i, R)
            a[own, :] = new_weight(a[own, :], gus[0][layer, held], gus[1][layer, held], gd_ref[layer, held])

    places = (n0_ref.at[0], n1_ref.at[0], nd_ref.at[0], nd_ref.at[1])
    new_down = [copy(a.at[pl.ds(i % 2 * R2, R2)], place, nsem.at[i]) for i, place in enumerate(places)]
    start(*new_down)
    for q, (e, layer) in enumerate(chunks):
        right_of(q).wait_recv()
        if e == 0:
            start(across(q))
        start(over(q, 1))
        left_of(q).wait_recv()
        if e:
            start(across(q))
        start(over(q, 2))
    for q in (0, 2, 1, 3):
        across(q).wait_recv()
        start(over(q, 3))
    wait(*new_down, *leaving)
    for q in range(len(chunks)):
        wait(*[over(q, i) for i in range(4)])
        for sent in (right_of(q), left_of(q), across(q)):
            sent.wait_send()


def copy_kernel(og_ref, ou_ref, ng_ref, nu_ref, buf, isem, osem):
    n, rows = buf.shape[:2]
    per = n // 2
    ins, outs = [], []
    for i in range(n):
        src, dst = ((og_ref, ng_ref), (ou_ref, nu_ref))[i // per]
        at = pl.ds(i % per * rows, rows)
        ins.append(copy(src.at[at], buf.at[i], isem.at[i]))
        outs.append(copy(buf.at[i], dst.at[at], osem.at[i]))
    start(*ins)
    for i in range(n):
        wait(ins[i])
        start(outs[i])
    wait(*outs)


def moments_kernel(fac_ref, *refs):
    ins, outs = refs[:9], refs[9:]
    for i in range(3):
        m, v, g = (r[0] for r in ins[3 * i : 3 * i + 3])
        g = g.astype(F32) * fac_ref[:1, :1]
        outs[2 * i][0] = 0.9 * m + 0.1 * g
        outs[2 * i + 1][0] = 0.95 * v + 0.05 * g * g


def place_kernel(firsts, at_ref, *refs):
    out, sem = refs[-2:]
    copies = []
    for i, first in enumerate(firsts):
        count, rows = refs[i].shape[:2]
        copies.append(copy(refs[i], out.at[pl.ds(first, count), pl.ds(pl.multiple_of(at_ref[i] * rows, 16), rows)], sem.at[i]))
    start(*copies)
    wait(*copies)


VMEM, HBM = pl.BlockSpec(memory_space=pltpu.VMEM), pl.BlockSpec(memory_space=pl.ANY)
dma = pltpu.SemaphoreType.DMA


def bf16(*shape):
    return pltpu.VMEM(shape, BF16)


def f32(*shape):
    return pltpu.VMEM(shape, F32)


def call(kernel, ins, out, scratch, cost, limit=VMEM_LIMIT, **params):
    flops, moved = cost
    more = {key: params.pop(key) for key in ("grid", "input_output_aliases") if key in params}
    outs = [spec for _, _, spec in out]
    shapes = [jax.ShapeDtypeStruct(shape, dtype) for shape, dtype, _ in out]
    return pl.pallas_call(
        kernel,
        out_shape=shapes,
        in_specs=ins,
        out_specs=outs,
        scratch_shapes=scratch,
        compiler_params=pltpu.CompilerParams(vmem_limit_bytes=limit, **params),
        cost_estimate=pl.CostEstimate(flops=int(flops), bytes_accessed=int(moved), transcendentals=0),
        **more,
    )


def solution(mesh):
    n = mesh.shape["dp"]
    chips = n // 2

    def ring(shift, flip=0):
        return [(i, (i // 2 + shift) % chips * 2 + (i + flip) % 2) for i in range(n)]

    def right(t):
        return lax.ppermute(t, "dp", ring(1))

    def left(t):
        return lax.ppermute(t, "dp", ring(-1))

    def partner(t):
        return lax.ppermute(t, "dp", ring(0, 1))

    def step(x, dy, *arrays):
        weights, m, v = (arrays[i : i + 3] for i in (0, 3, 6))
        wg, wu, wd = weights
        T, D = x.shape[1:]
        layers, _, FF = wg.shape
        W, CH = D, 512
        NT, NC, R = FF // W, T // CH, D // n
        NS = FF // n // R
        z = SimpleNamespace(T=T, D=D, FF=FF, W=W, CH=CH, NT=NT, NC=NC, R=R, NS=NS, chips=chips, count=float(sum(w.size for w in weights)))
        tokens, turned, hidden = ((T, D), BF16, HBM), ((D, T), BF16, HBM), ((layers, NT, T, W), BF16, HBM)
        h1, a1, a1T, a0, a0T, dyT, hid = call(
            functools.partial(forward_kernel, z), [HBM] * 5,
            [tokens, tokens, turned, tokens, turned, turned, hidden],
            [*[bf16(T, D)] * 3, *[bf16(D, T)] * 2, *[bf16(T, D)] * 2, bf16(D, T), bf16(2, D, 2 * W), bf16(FF, D), bf16(T, FF), *[f32(2, CH, W)] * 2,
             dma((2, 2)), dma((3,)), dma((NT,)), dma((NC + 1, 3))],
            (6 * T * D * FF, 8 * T * FF),
        )(x, dy, wg, wu, wd)
        slots = 6 + NS
        blocks = bf16(slots, R, W)
        flat, tall, half, gathered = (layers, R, FF), (layers, NS * R, D), (1, NS * R, D), (layers, D, FF)
        gg, gup, gd, fac, nd, n0, n1, og, ou, _ = call(
            functools.partial(backward_kernel, z), [HBM] * 17,
            [(flat, BF16, HBM), (flat, BF16, HBM), (tall, BF16, HBM), ((8, 128), F32, HBM), (tall, BF16, HBM), (half, BF16, HBM), (half, BF16, HBM),
             (gathered, BF16, HBM), (gathered, BF16, HBM), hidden],
            [bf16(T, D), bf16(D, T), bf16(T, D), bf16(D, T), bf16(2, D, 2 * W), bf16(2, W, D), *[f32(2, CH, W)] * 4, *[bf16(CH, W)] * 2,
             bf16(2, T, W), bf16(T, 2 * W),
             bf16(slots, chips, 2, R, W), bf16(slots, chips, R, W), blocks, blocks, blocks, bf16(*flat), bf16(*flat), bf16(*tall), f32(8, 128),
             f32(8, W), f32(n, 8, 128),
             dma((2, 2)), dma((2,)), dma((4,)), dma((2,)), *[dma((slots,))] * 8, dma((n,)), dma((n,)),
             *[dma((4,))] * 9, *[dma((4, 4))] * 2],
            (24 * T * D * FF, 8 * T * FF), collective_id=0, has_side_effects=True, input_output_aliases={16: 9},
        )(h1, a1, a1T, a0, a0T, dyT, dy, wg, wu, wd, m[0], v[0], m[1], v[1], m[2], v[2], hid)

        me = lax.axis_index("dp")
        c, k = me // 2, lax.rem(me, 2)

        def place(out, pieces):
            ts = [t for t, _, _ in pieces]
            count = len(ts)
            known = () if out is None else (out,)
            return call(
                functools.partial(place_kernel, [first for _, _, first in pieces]),
                [pl.BlockSpec(memory_space=pltpu.SMEM)] + [VMEM] * count + [HBM] * len(known), [(wd.shape, BF16, HBM)], [dma((count,))],
                (2e6 * count, 4 * sum(t.size for t in ts)), 1 << 24, input_output_aliases={count + 1: 0} if known else {},
            )(jnp.stack([at for _, at, _ in pieces]).astype(jnp.int32), *ts, *known)[0]

        def spot(shift, core):
            return lax.rem(c + shift + chips, chips) * 2 + core

        left0, right1 = right(n0), left(n1)
        left1, right0 = right(n1), left(n0)
        p_own = partner(nd)
        rows = layers * D
        parts = [(rows, FF), BF16, HBM]
        ng, nu = call(
            copy_kernel, [HBM] * 2, [parts] * 2, [bf16(8, rows // 4, FF), dma((8,)), dma((8,))], (12e9, 8 * rows * FF),
        )(og.reshape(rows, FF), ou.reshape(rows, FF))
        opp = right(left0), left(right1)
        kinds = [(shape, pl.BlockSpec((1, *shape[1:]), lambda i: (i, 0, 0))) for shape in (flat, flat, tall)]
        moved = call(
            moments_kernel, [pl.BlockSpec((8, 128), lambda i: (0, 0))] + [spec for _, spec in kinds for _ in range(3)],
            [(shape, F32, spec) for shape, spec in kinds for _ in range(2)], [], (10e9, 54 * m[0].size), grid=(layers,),
        )(fac, *[t for i, g in enumerate((gg, gup, gd)) for t in (m[i], v[i], g)])
        p_sides = [partner(t) for t in (left0, right1, left1, right0)]
        pieces = [(nd, spot(0, k), 0), (p_own, spot(0, 1 - k), 0)]
        for t, p, (j, first) in zip((left0, right1, left1, right0), p_sides, ((-1, 0), (1, 1), (-1, 1), (1, 0)), strict=True):
            pieces += [(t, spot(j, k), first), (p, spot(j, 1 - k), first)]
        out = place(None, pieces)
        p_opp = [partner(t) for t in opp]
        out = place(out, [piece for i in range(2) for piece in ((opp[i], spot(2, k), i), (p_opp[i], spot(2, 1 - k), i))])
        return ng.reshape(gathered), nu.reshape(gathered), out, *moved[::2], *moved[1::2]

    whole, split = P(None, None, None), P(None, "dp", None)
    step = jax.shard_map(
        step,
        mesh=mesh,
        in_specs=(P(("rep", "dp")),) * 2 + (whole,) * 3 + (split,) * 6,
        out_specs=(P("rep", None, None),) * 3 + (P("rep", "dp", None),) * 6,
        check_vma=False,
    )
    return step
```

```python
import functools
from types import SimpleNamespace

import jax
import jax.numpy as jnp
from jax import lax
from jax.experimental import pallas as pl
from jax.experimental.pallas import tpu as pltpu
from jax.sharding import PartitionSpec as P

F32, BF16 = jnp.float32, jnp.bfloat16
VMEM_LIMIT = 67043328
NT_DIMS = (((1,), (1,)), ((), ()))
copy = pltpu.make_async_copy


def dot(a, b):
    return jnp.dot(a, b, preferred_element_type=F32)


def dot_nt(a, b):
    return lax.dot_general(a, b, NT_DIMS, preferred_element_type=F32)


def sigmoid(g):
    return 0.5 * jnp.tanh(0.5 * g) + 0.5


def scale_of(h):
    return lax.rsqrt(jnp.mean(h * h, -1, keepdims=True) + 1e-6)


def span(i, n):
    return pl.ds(pl.multiple_of(i * n, n), n)


def start(*copies):
    for c in copies:
        c.start()


def wait(*copies):
    for c in copies:
        c.wait()


def step_kernel(z, x_ref, dy_ref, wg_ref, wu_ref, wd_ref, mg_ref, vg_ref, mu_ref, vu_ref, md_ref, vd_ref,
                    gg_out, gup_out, gd_out, fac_out, nd_ref, n0_ref, n1_ref, og_ref, ou_ref, hid_ref, h1_ref, a0_ref, a0T_ref,
                    a, aT, dy, dyT, wgu, wd, gu0, gu1, gu2, gu3, dh0, dh1, hids, dgu,
                    G, PB, OB, B1, B2, gg_ref, gup_ref, gd_ref, fac_ref, ssacc, ssall,
                    wsem, dsem, tsem, hsem, sP, rP, sO, rO, s1, r1, s2, r2, sS, rS,
                    msem, nsem, lsem, sR, rR, sL, rL, sX, rX, sD, rD):
    W, CH, NT, NC, T, D, R, NS = z.W, z.CH, z.NT, z.NC, z.T, z.D, z.R, z.NS
    NA = 6
    peers = 2 * z.chips
    gus, dhs = (gu0, gu1, gu2, gu3), (dh0, dh1)
    rep, me = lax.axis_index("rep"), lax.axis_index("dp")
    c, k = me // 2, lax.rem(me, 2)

    def chip(j):
        return lax.rem(c + j + z.chips, z.chips)

    def remote(src, dst, send, recv, to):
        return pltpu.make_async_remote_copy(src_ref=src, dst_ref=dst, send_sem=send, recv_sem=recv, device_id=(rep, to),
                                            device_id_type=pl.DeviceIdType.MESH)

    bar = pltpu.get_barrier_semaphore()
    for j in range(1, peers):
        pl.semaphore_signal(bar, inc=1, device_id=(rep, lax.rem(me + j, peers)), device_id_type=pl.DeviceIdType.MESH)

    partner = c * 2 + 1 - k

    def copyP(s):
        return remote(G.at[s, :, 1 - k], PB.at[s], sP.at[s], rP.at[s], partner)

    def copyO(s, d):
        return remote(G.at[s, chip(2), k], OB.at[s], sO.at[s], rO.at[s], chip(d) * 2 + k)

    def copy1(s, d):
        return remote(G.at[s, chip(-d), k], B1.at[s], s1.at[s], r1.at[s], chip(-d) * 2 + k)

    def copy2(s, d):
        return remote(G.at[s, chip(d), k], B2.at[s], s2.at[s], r2.at[s], chip(d) * 2 + k)

    def both(s, q):
        return G[s, q, k].astype(F32) + PB[s, q].astype(F32)

    def stage0(each):
        each(lambda s, d, put: copyP(s).start())

    def stage1(each):
        def add(s, d, put):
            for q in (chip(2), chip(-d)):
                G[s, q, k] = both(s, q).astype(BF16)

        each(lambda s, d, put: copyP(s).wait_recv())
        each(add)
        each(lambda s, d, put: copyO(s, d).start())
        each(lambda s, d, put: copy1(s, d).start())

    def stage2(each):
        def add(s, d, put):
            q = chip(d)
            G[s, q, k] = (both(s, q) + OB[s].astype(F32)).astype(BF16)

        each(lambda s, d, put: copyO(s, d).wait_recv())
        each(add)
        each(lambda s, d, put: copy2(s, d).start())

    def stage3(each):
        def arrive(s, d, put):
            copy1(s, d).wait_recv()
            copy2(s, d).wait_recv()

        def add(s, d, put):
            g = (both(s, c) + (B1[s].astype(F32) + B2[s].astype(F32))).astype(BF16)
            put(g)
            w = g.astype(F32)
            ssacc[...] += jnp.sum((w * w).reshape(-1, *ssacc.shape), 0)

        def sent(s, d, put):
            for cp in (copyP(s), copyO(s, d), copy1(s, d), copy2(s, d)):
                cp.wait_send()

        for f in (arrive, add, sent):
            each(f)

    stages = stage0, stage1, stage2, stage3

    def a_slot(r, e):
        return lax.rem(r * 2 + e, NA)

    def a_put(r, e):
        def put(g):
            (gg_ref, gup_ref)[e][1 - r // NT, :, span(lax.rem(r, NT), W)] = g

        return put

    def stream_a(stage, r):
        stages[stage](lambda f: [f(a_slot(r, e), d, a_put(r, e)) for e, d in enumerate((1, -1))])

    def stream_b(stage, layer):
        def put(i):
            def f(g):
                gd_ref[layer, span(i, R), :] = g

            return f

        stages[stage](lambda f: pl.loop(0, NS)(lambda i: f(NA + i, lax.rem(i + layer, 2) * 2 - 1, put(i))))

    def tiles(g):
        slot, layer, t = lax.rem(g, 2), lax.rem(g // NT, 2), lax.rem(g, NT)
        sides = [copy(ref.at[layer, :, span(t, W)], wgu.at[slot, :, pl.ds(e * W, W)], wsem.at[slot, e]) for e, ref in enumerate((wg_ref, wu_ref))]
        return [*sides, copy(wd_ref.at[layer, span(t, W), :], wd.at[slot], dsem.at[slot])]

    def hid_out(t):
        return copy(hids.at[0], hid_ref.at[1, t], hsem.at[0])

    def gate_up_grads(r):
        for j in range(0, 2 * W, 256):
            gw = dot(aT[...], dgu[:, j : j + 256]).astype(BF16)
            for i in range(0, 256, 128):
                e, q = divmod(j + i, W)
                G[a_slot(r, e), :, :, :, q : q + 128] = gw[:, i : i + 128].reshape(*G.shape[1:4], 128)

    def hid_in(layer, i, slot):
        return copy(hid_ref.at[layer, NT - 1 - i], hids.at[lax.rem(slot, 2)], hsem.at[lax.rem(slot, 2)])

    def turn_units(sd, i):
        for j in range(0, W, 128):
            rows = sd[:, j : j + 128].T
            for b in range(8):
                lo, hi = max(j, b * R), min(j + 128, b * R + R)
                if lo < hi:
                    B = (NT - 1 - i) * 8 + b
                    unit = G.at[NA + lax.rem(B, NS), B // (2 * NS), lax.rem(B // NS, 2)]
                    unit[lo - b * R : hi - b * R] = rows[lo - j : hi - j]

    def down_grads(r, layer, sd):
        def product(i):
            for j in range(0, W, 256):
                n = min(256, W - j)
                sd[:, j : j + n] = dot(dyT[...], hids[lax.rem(i, 2), :, j : j + n]).astype(BF16)
            start(hid_in(layer, jnp.minimum(i + 2, NT - 1), i))

        product(0)
        stream_a(1, r)

        @pl.loop(1, NT)
        def _(i):
            wait(hid_in(layer, i, i))
            turn_units(sd, i - 1)
            product(i)

        turn_units(sd, NT - 1)
        stream_b(0, layer)
        stream_a(3, r - 1)
        wait(hid_in(layer, 0, 0), hid_in(layer, 0, 1))

    def da_at(ci):
        return (gu2, gu3)[ci // 2].at[ci % 2]

    def output_grad(ci):
        step = CH // 2

        @pl.loop(0, 2)
        def _(j):
            r = span(ci * 2 + j, step)
            h = dgu[r, :W].astype(F32)
            s = scale_of(h)
            d = da_at(ci)[span(j, step), :].astype(BF16).astype(F32)
            n = dy[r, :] + (s * (d - h * (s * s * jnp.mean(d * h, -1, keepdims=True)))).astype(BF16)
            dy[r, :] = n
            dyT[:, r] = n.T

    swap = [copy(s, d, tsem.at[i]) for i, (s, d) in enumerate(((h1_ref, dgu.at[:, pl.ds(0, W)]), (a0_ref, a), (a0T_ref, aT)))]

    def turn():
        wait(*swap)
        output_grad(0)
        output_grad(1)
        output_grad(2)
        output_grad(3)
        stream_a(2, NT - 1)
        stream_b(1, 1)

    ins = [copy(x_ref.at[0], dgu.at[:, pl.ds(0, W)], tsem.at[0]), copy(dy_ref.at[0], dy, tsem.at[1])]
    start(ins[0], *tiles(0), ins[1])
    ssacc[...] = jnp.zeros_like(ssacc)
    for ci in range(NC):
        da_at(ci)[...] = jnp.zeros((CH, D), F32)
    wait(ins[0])
    step = CH // 2
    for i in range(T // step):
        rows = pl.ds(i * step, step)
        h = dgu[rows, :W].astype(F32)
        a[rows, :] = (h * scale_of(h)).astype(BF16)
    keep_a, keep_aT = copy(a, a0_ref, tsem.at[0]), copy(aT, a0T_ref, tsem.at[2])
    start(keep_a)
    wait(ins[1])

    def first_out(t):
        return copy(hids.at[lax.rem(t, 2)], hid_ref.at[0, t], hsem.at[lax.rem(t, 2)])

    @pl.loop(0, NT)
    def _(t):
        slot = lax.rem(t, 2)
        wait(*tiles(t))
        start(*tiles(t + 1))

        @pl.when(t >= 2)
        def _():
            wait(first_out(t - 2))

        turned = span(jnp.minimum(t, NC - 1), CH)
        aT[:, turned] = a[turned, :].T
        dyT[:, turned] = dy[turned, :].T

        def E(ci):
            rows = pl.ds(ci * CH, CH)
            g, u = gus[ci % 2][0], gus[ci % 2][1]
            hids[slot, rows, :] = (g * sigmoid(g) * u).astype(BF16)
            da_at(ci)[...] += dot(hids[slot, rows, :], wd[slot])

        for ci in range(NC):
            gu = dot(a[pl.ds(ci * CH, CH), :], wgu[slot])
            gus[ci % 2][0] = gu[:, :W]
            gus[ci % 2][1] = gu[:, W:]
            if ci:
                E(ci - 1)
        E(NC - 1)
        start(first_out(t))

    start(keep_aT)
    wait(keep_a)
    for i, ref in enumerate((gu2, gu3)):
        @pl.loop(0, 2)
        def _(j):
            rows = span(i * 2 + j, CH)
            y = dgu[rows, :W] + ref[j].astype(BF16)
            dgu[rows, W:] = y
            h = y.astype(F32)
            a[rows, :] = (h * scale_of(h)).astype(BF16)
            ref[j] = jnp.zeros((CH, D), F32)

    keep_h = copy(dgu.at[:, pl.ds(W, W)], h1_ref, tsem.at[3])
    start(keep_h)
    wait(keep_aT)

    @pl.loop(0, NC)
    def _(i):
        aT[:, span(i, CH)] = a[span(i, CH), :].T

    wait(keep_h, first_out(NT - 2), first_out(NT - 1))

    @pl.loop(0, 2 * NT)
    def _(r):
        g = r + NT
        slot = lax.rem(g, 2)
        wait(*tiles(g))

        @pl.when(r + 1 < 2 * NT)
        def _():
            start(*tiles(g + 1))

        @pl.when((r >= 1) & (r < NT))
        def _():
            wait(hid_out(r - 1))

        def A(ci):
            rows = pl.ds(ci * CH, CH)
            gu = dot(a[rows, :], wgu[slot])
            gus[ci % 2][0] = gu[:, :W]
            gus[ci % 2][1] = gu[:, W:]
            dhs[ci % 2][...] = dot_nt(dy[rows, :], wd[slot]).astype(BF16)

        def E(ci):
            rows = pl.ds(ci * CH, CH)
            gu = gus[ci % 2]
            g, u, d = gu[0], gu[1], dhs[ci % 2][...].astype(F32)
            s = sigmoid(g)
            silu = g * s
            hids[r // NT, rows, :] = (silu * u).astype(BF16)
            dgu[rows, :W] = (d * u * (s + silu * (1.0 - s))).astype(BF16)
            dgu[rows, W:] = (d * silu).astype(BF16)

        for ci in range(NC):
            A(ci)
            if ci:
                E(ci - 1)

        @pl.when(r == 0)
        def _():
            pl.semaphore_wait(bar, peers - 1)

        usual = (r != NT) & (r != NT + 2)

        @pl.when((r >= 1) & usual)
        def _():
            stream_a(1, r - 1)

            @pl.when(r >= 2)
            def _():
                stream_a(3, r - 2)

            @pl.when(r == NT + 1)
            def _():
                start(hid_in(0, 0, 0))
                stream_b(3, 1)

        @pl.when(r == NT + 2)
        def _():
            stream_b(1, 0)

        E(NC - 1)
        gate_up_grads(r)
        stream_a(0, r)

        @pl.when(r < NT - 1)
        def _():
            start(hid_out(r))

        @pl.when(r < NT)
        def _():
            for ci in range(NC):
                da_at(ci)[...] += dot_nt(dgu[pl.ds(ci * CH, CH), :], wgu[slot])

        @pl.when((r >= 1) & usual)
        def _():
            stream_a(2, r - 1)

        @pl.when((r >= NT - 1) & (r < NT + 4))
        def _():
            @pl.when(r == NT)
            def _():
                stream_b(2, 1)

            @pl.when(r == NT + 3)
            def _():
                stream_b(2, 0)

            @pl.when((r == NT - 1) | (r == NT + 1))
            def _():
                layer = (NT + 1 - r) // 2

                @pl.when(layer == 1)
                def _():
                    start(*swap, hid_in(1, 1, 1))

                @pl.when(layer == 0)
                def _():
                    start(hid_in(0, 1, 1))
                    wait(hid_in(0, 0, 0))

                down_grads(r, layer, wd.at[slot])

                @pl.when(layer == 1)
                def _():
                    turn()

                @pl.when(layer == 0)
                def _():
                    stream_a(2, r)

    R2 = NS * R

    def block(ref, i, layer, t):
        return ref.at[layer, span(i, R), span(t, W)]

    def nw(e, layer, t):
        return hids.at[e, span(layer * NT + t, R)]

    @pl.loop(0, NT)
    def _(t):
        for layer in range(2):
            for i, ref in enumerate((mg_ref, vg_ref, mu_ref, vu_ref)):
                start(copy(block(ref, 0, layer, t), gus[i].at[layer, span(t, R)], msem.at[i]))
            for e, ref in enumerate((wg_ref, wu_ref)):
                start(copy(block(ref, me, layer, t), nw(e, layer, t), nsem.at[e]))

    def arrived(ref, sem):
        wait(copy(ref, ref, sem))

    own_down = [copy(wd_ref.at[layer, span(me, R2), :], a.at[pl.ds(layer * R2, R2)], nsem.at[2 + layer]) for layer in range(2)]
    start(*own_down)

    last = 2 * NT - 1
    stream_a(1, last)
    stream_a(3, last - 1)
    stream_a(2, last)
    stream_b(3, 0)
    stream_a(3, last)

    lanes = ssall.shape[-1]
    part = ssacc[:, :lanes]
    for j in range(1, W // lanes):
        part = part + ssacc[:, j * lanes : (j + 1) * lanes]
    ssall[me] = part
    parts = [remote(ssall.at[me], ssall.at[me], sS.at[j], rS.at[j], lax.rem(me + j, peers)) for j in range(1, peers)]
    start(*parts)
    wait(*parts)
    total = ssall[0]
    for j in range(1, peers):
        total = total + ssall[j]
    total = jnp.sum(jnp.sum(total, 0, keepdims=True), 1, keepdims=True)
    fac = jnp.minimum(1.0, 0.5 * lax.rsqrt(total / z.count + 1e-30))
    fac_ref[...] = jnp.broadcast_to(fac, fac_ref.shape)
    pairs = (gg_ref, gg_out), (gup_ref, gup_out), (gd_ref, gd_out), (fac_ref, fac_out)
    leaving = [copy(s, d, tsem.at[i]) for i, (s, d) in enumerate(pairs)]
    start(*leaving)

    def new_weight(w, m, v, g):
        w, g = w.astype(F32), g.astype(F32) * fac
        m = 0.9 * m + 0.1 * g
        v = 0.95 * v + 0.05 * g * g
        return (w - 0.02 * (m * lax.rsqrt(v + 1e-8) + 0.1 * w)).astype(BF16)

    outs = (og_ref, ou_ref)
    chunks = [(e, layer) for e in range(2) for layer in range(2)]

    def here(q, j):
        e, layer = chunks[q]
        return outs[e].at[layer, span(chip(j) * 2 + k, R)]

    def send(q, j, send, recv, to):
        return remote(here(q, j), here(q, j), send, recv, to)

    def right_of(q):
        return send(q, 0, sR.at[q], rR.at[q], chip(1) * 2 + k)

    def left_of(q):
        return send(q, 0, sL.at[q], rL.at[q], chip(-1) * 2 + k)

    def across(q):
        j = chunks[q][0] * 2 - 1
        return send(q, j, sX.at[q], rX.at[q], chip(-j) * 2 + k)

    def over(q, i):
        return send(q, (0, -1, 1, 2)[i], sD.at[q, i], rD.at[q, i], partner)

    def leave(q):
        arrived(here(q, 0), lsem.at[q])
        start(right_of(q), left_of(q), over(q, 0))

    for q, (e, layer) in enumerate(chunks):
        if layer == 0:
            arrived(hids.at[e, pl.ds(0, 2 * NT * R)], nsem.at[e])
            for i in (2 * e, 2 * e + 1):
                arrived(gus[i].at[:, pl.ds(0, NT * R)], msem.at[i])

        @pl.loop(0, NT)
        def _(t):
            held = span(t, R)
            own = nw(e, layer, t)
            own[...] = new_weight(own[...], gus[2 * e][layer, held], gus[2 * e + 1][layer, held], (gg_ref, gup_ref)[e][layer, :, span(t, W)])
            start(copy(own, block(outs[e], me, layer, t), lsem.at[q]))

        if q:
            leave(q - 1)
    leave(len(chunks) - 1)
    moments = [copy(ref, gus[i].at[:, pl.ds(0, R2)], msem.at[i]) for i, ref in enumerate((md_ref, vd_ref))]
    start(*moments)
    wait(*own_down, *moments)

    @pl.loop(0, NS)
    def _(i):
        for layer in range(2):
            held, own = span(i, R), span(layer * NS + i, R)
            a[own, :] = new_weight(a[own, :], gus[0][layer, held], gus[1][layer, held], gd_ref[layer, held])

    places = (n0_ref.at[0], n1_ref.at[0], nd_ref.at[0], nd_ref.at[1])
    new_down = [copy(a.at[pl.ds(i % 2 * R2, R2)], place, nsem.at[i]) for i, place in enumerate(places)]
    start(*new_down)
    for q, (e, layer) in enumerate(chunks):
        right_of(q).wait_recv()
        if e == 0:
            start(across(q))
        start(over(q, 1))
        left_of(q).wait_recv()
        if e:
            start(across(q))
        start(over(q, 2))
    for q in (0, 2, 1, 3):
        across(q).wait_recv()
        start(over(q, 3))
    wait(*new_down, *leaving)
    for q in range(len(chunks)):
        wait(*[over(q, i) for i in range(4)])
        for sent in (right_of(q), left_of(q), across(q)):
            sent.wait_send()


def copy_kernel(og_ref, ou_ref, ng_ref, nu_ref, buf, isem, osem):
    n, rows = buf.shape[:2]
    per = n // 2
    ins, outs = [], []
    for i in range(n):
        src, dst = ((og_ref, ng_ref), (ou_ref, nu_ref))[i // per]
        at = pl.ds(i % per * rows, rows)
        ins.append(copy(src.at[at], buf.at[i], isem.at[i]))
        outs.append(copy(buf.at[i], dst.at[at], osem.at[i]))
    start(*ins)
    for i in range(n):
        wait(ins[i])
        start(outs[i])
    wait(*outs)


def moments_kernel(fac_ref, *refs):
    ins, outs = refs[:9], refs[9:]
    for i in range(3):
        m, v, g = (r[0] for r in ins[3 * i : 3 * i + 3])
        g = g.astype(F32) * fac_ref[:1, :1]
        outs[2 * i][0] = 0.9 * m + 0.1 * g
        outs[2 * i + 1][0] = 0.95 * v + 0.05 * g * g


def place_kernel(firsts, at_ref, *refs):
    out, sem = refs[-2:]
    copies = []
    for i, first in enumerate(firsts):
        count, rows = refs[i].shape[:2]
        copies.append(copy(refs[i], out.at[pl.ds(first, count), pl.ds(pl.multiple_of(at_ref[i] * rows, 16), rows)], sem.at[i]))
    start(*copies)
    wait(*copies)


VMEM, HBM = pl.BlockSpec(memory_space=pltpu.VMEM), pl.BlockSpec(memory_space=pl.ANY)
dma = pltpu.SemaphoreType.DMA


def bf16(*shape):
    return pltpu.VMEM(shape, BF16)


def f32(*shape):
    return pltpu.VMEM(shape, F32)


def call(kernel, ins, out, scratch, cost, limit=VMEM_LIMIT, **params):
    flops, moved = cost
    more = {key: params.pop(key) for key in ("grid", "input_output_aliases") if key in params}
    outs = [spec for _, _, spec in out]
    shapes = [jax.ShapeDtypeStruct(shape, dtype) for shape, dtype, _ in out]
    return pl.pallas_call(
        kernel,
        out_shape=shapes,
        in_specs=ins,
        out_specs=outs,
        scratch_shapes=scratch,
        compiler_params=pltpu.CompilerParams(vmem_limit_bytes=limit, **params),
        cost_estimate=pl.CostEstimate(flops=int(flops), bytes_accessed=int(moved), transcendentals=0),
        **more,
    )


def solution(mesh):
    n = mesh.shape["dp"]
    chips = n // 2

    def ring(shift, flip=0):
        return [(i, (i // 2 + shift) % chips * 2 + (i + flip) % 2) for i in range(n)]

    def right(t):
        return lax.ppermute(t, "dp", ring(1))

    def left(t):
        return lax.ppermute(t, "dp", ring(-1))

    def partner(t):
        return lax.ppermute(t, "dp", ring(0, 1))

    def step(x, dy, *arrays):
        weights, m, v = (arrays[i : i + 3] for i in (0, 3, 6))
        wg, wu, wd = weights
        T, D = x.shape[1:]
        layers, _, FF = wg.shape
        W, CH = D, 512
        NT, NC, R = FF // W, T // CH, D // n
        NS = FF // n // R
        z = SimpleNamespace(T=T, D=D, FF=FF, W=W, CH=CH, NT=NT, NC=NC, R=R, NS=NS, chips=chips, count=float(sum(w.size for w in weights)))
        tokens = (T, D), BF16, HBM
        slots = 6 + NS
        blocks = bf16(slots, R, W)
        flat, tall, half, gathered = (layers, R, FF), (layers, NS * R, D), (1, NS * R, D), (layers, D, FF)
        gg, gup, gd, fac, nd, n0, n1, og, ou, *_ = call(
            functools.partial(step_kernel, z), [HBM] * 11,
            [(flat, BF16, HBM), (flat, BF16, HBM), (tall, BF16, HBM), ((8, 128), F32, HBM), (tall, BF16, HBM), (half, BF16, HBM), (half, BF16, HBM),
             (gathered, BF16, HBM), (gathered, BF16, HBM), ((layers, NT, T, W), BF16, HBM), tokens, tokens, ((D, T), BF16, HBM)],
            [bf16(T, D), bf16(D, T), bf16(T, D), bf16(D, T), bf16(2, D, 2 * W), bf16(2, W, D), *[f32(2, CH, W)] * 4, *[bf16(CH, W)] * 2,
             bf16(2, T, W), bf16(T, 2 * W),
             bf16(slots, chips, 2, R, W), bf16(slots, chips, R, W), blocks, blocks, blocks, bf16(*flat), bf16(*flat), bf16(*tall), f32(8, 128),
             f32(8, W), f32(n, 8, 128),
             dma((2, 2)), dma((2,)), dma((4,)), dma((2,)), *[dma((slots,))] * 8, dma((n,)), dma((n,)),
             *[dma((4,))] * 9, *[dma((4, 4))] * 2],
            (30 * T * D * FF, 8 * T * FF), collective_id=0, has_side_effects=True,
        )(x, dy, wg, wu, wd, m[0], v[0], m[1], v[1], m[2], v[2])

        me = lax.axis_index("dp")
        c, k = me // 2, lax.rem(me, 2)

        def place(out, pieces):
            ts = [t for t, _, _ in pieces]
            count = len(ts)
            known = () if out is None else (out,)
            return call(
                functools.partial(place_kernel, [first for _, _, first in pieces]),
                [pl.BlockSpec(memory_space=pltpu.SMEM)] + [VMEM] * count + [HBM] * len(known), [(wd.shape, BF16, HBM)], [dma((count,))],
                (2e6 * count, 4 * sum(t.size for t in ts)), 1 << 24, input_output_aliases={count + 1: 0} if known else {},
            )(jnp.stack([at for _, at, _ in pieces]).astype(jnp.int32), *ts, *known)[0]

        def spot(shift, core):
            return lax.rem(c + shift + chips, chips) * 2 + core

        left0, right1 = right(n0), left(n1)
        left1, right0 = right(n1), left(n0)
        p_own = partner(nd)
        rows = layers * D
        parts = [(rows, FF), BF16, HBM]
        ng, nu = call(
            copy_kernel, [HBM] * 2, [parts] * 2, [bf16(8, rows // 4, FF), dma((8,)), dma((8,))], (12e9, 8 * rows * FF),
        )(og.reshape(rows, FF), ou.reshape(rows, FF))
        opp = right(left0), left(right1)
        kinds = [(shape, pl.BlockSpec((1, *shape[1:]), lambda i: (i, 0, 0))) for shape in (flat, flat, tall)]
        moved = call(
            moments_kernel, [pl.BlockSpec((8, 128), lambda i: (0, 0))] + [spec for _, spec in kinds for _ in range(3)],
            [(shape, F32, spec) for shape, spec in kinds for _ in range(2)], [], (10e9, 54 * m[0].size), grid=(layers,),
        )(fac, *[t for i, g in enumerate((gg, gup, gd)) for t in (m[i], v[i], g)])
        p_sides = [partner(t) for t in (left0, right1, left1, right0)]
        pieces = [(nd, spot(0, k), 0), (p_own, spot(0, 1 - k), 0)]
        for t, p, (j, first) in zip((left0, right1, left1, right0), p_sides, ((-1, 0), (1, 1), (-1, 1), (1, 0)), strict=True):
            pieces += [(t, spot(j, k), first), (p, spot(j, 1 - k), first)]
        out = place(None, pieces)
        p_opp = [partner(t) for t in opp]
        out = place(out, [piece for i in range(2) for piece in ((opp[i], spot(2, k), i), (p_opp[i], spot(2, 1 - k), i))])
        return ng.reshape(gathered), nu.reshape(gathered), out, *moved[::2], *moved[1::2]

    whole, split = P(None, None, None), P(None, "dp", None)
    step = jax.shard_map(
        step,
        mesh=mesh,
        in_specs=(P(("rep", "dp")),) * 2 + (whole,) * 3 + (split,) * 6,
        out_specs=(P("rep", None, None),) * 3 + (P("rep", "dp", None),) * 6,
        check_vma=False,
    )
    return step
```
